8 devices in a mesh: dp: 2 (over z, y), ep: 4 (over x, core).
Axes of the slice: x: 2, y: 2, z: 1, core: 2. Of those that a mesh axis runs over, the one named last changes fastest.
Arguments:
- tokens: bfloat16 [2048, 2048], P(('dp', 'ep')), parts along dimension 0
- expert_ids: int32 [2048, 2], P(('dp', 'ep')), parts along dimension 0
- gate_w: float32 [2048, 2], P(('dp', 'ep')), parts along dimension 0
- route_counts: int32 [8, 8], P(('dp', 'ep')), parts along dimension 0
- w_gate: bfloat16 [8, 2048, 5632], P('ep')
- w_up: bfloat16 [8, 2048, 5632], P('ep')
- w_down: bfloat16 [8, 5632, 2048], P('ep')
Outputs:
- output: bfloat16 [2048, 2048], P(('dp', 'ep')), parts along dimension 0
There are 2 independent parts. The reference program is written for one: setup_inputs(seed, part) draws one part's arguments, and reference() takes and returns one part's arrays. A program takes and returns all parts, laid end to end along the dimension named above; an argument that names none is the same for every part.
All inputs are finite; a program needn't handle non-finite values.
Results may differ from the reference program's by a relative error of at most 0.001.
Values are sent between devices in bfloat16 or wider.
A program may use at most 1 GiB of HBM per device.

```python
import jax
import jax.numpy as jnp
from jax import lax

GROUP_SIZE = 4
TOKENS_DEV = 256
MODEL_DIM = 2048
FFN_DIM = 5632
NUM_EXPERTS = 8
TOP_K = 2
CAPACITY = 128
HOT_DEVS = 1

LOCAL_EXPERTS = NUM_EXPERTS // GROUP_SIZE
GROUP_ROWS = GROUP_SIZE * TOKENS_DEV


def draw_routing(route_key):
    key_hot, key_star, key_noise, key_cover = jax.random.split(route_key, 4)
    expert_ar = jnp.arange(NUM_EXPERTS)
    expert_dev = expert_ar // LOCAL_EXPERTS
    hot_base = jax.random.randint(key_hot, (), 0, GROUP_SIZE)
    hot_list = (hot_base + jnp.arange(HOT_DEVS) * (GROUP_SIZE // HOT_DEVS)) % GROUP_SIZE
    is_hot = jnp.any(expert_dev[:, None] == hot_list[None, :], axis=1)
    star_expert = hot_base * LOCAL_EXPERTS + jax.random.randint(key_star, (), 0, LOCAL_EXPERTS)
    bonus_int = jnp.where(is_hot, 50, 0) + jnp.where(expert_ar == star_expert, 1000, 0)
    noise_int = jax.random.randint(key_noise, (GROUP_SIZE, TOKENS_DEV, NUM_EXPERTS), 0, 100)
    source = jnp.arange(GROUP_SIZE)
    tok_ar = jnp.arange(TOKENS_DEV)
    choice = jnp.arange(TOP_K)
    cover_rank = tok_ar[:, None] * (TOP_K - 1) + choice[None, :] - 1
    forced = (choice[None, :] >= 1) & (cover_rank < GROUP_SIZE - 1)
    cover_dev = (source[:, None, None] + 1 + cover_rank[None, :, :]) % GROUP_SIZE
    cover_exp = cover_dev * LOCAL_EXPERTS + jax.random.randint(key_cover, (GROUP_SIZE, TOKENS_DEV, TOP_K), 0, LOCAL_EXPERTS)
    taken_mask = jnp.any((cover_exp[:, :, :, None] == expert_ar) & forced[None, :, :, None], axis=2)
    home_mask = (expert_dev[None, :] == source[:, None])[:, None, :]
    pick_score = jnp.where(home_mask | taken_mask, -1, noise_int + bonus_int[None, None, :])
    ranked = lax.top_k(pick_score * NUM_EXPERTS + expert_ar, TOP_K)[1]
    n_forced = jnp.sum(forced.astype(jnp.int32), axis=1)
    pick_col = jnp.clip(jnp.where(choice[None, :] == 0, 0, choice[None, :] - n_forced[:, None]), 0, TOP_K - 1)
    free_exp = jnp.take_along_axis(ranked, jnp.broadcast_to(pick_col[None, :, :], ranked.shape), axis=2)
    expert_ids = jnp.where(forced[None, :, :], cover_exp, free_exp).astype(jnp.int32)
    onehot = (expert_ids.reshape(GROUP_SIZE, TOKENS_DEV * TOP_K, 1) == expert_ar).astype(jnp.int32)
    route_counts = jnp.minimum(jnp.sum(onehot, axis=1), CAPACITY).astype(jnp.int32)
    return expert_ids.reshape(GROUP_ROWS, TOP_K), route_counts


def setup_inputs(seed: int = 0, part: int = 0) -> dict:
    base_key = jax.random.key(seed)
    part_key = jax.random.fold_in(base_key, part)
    key_route, key_tok, key_gate = jax.random.split(part_key, 3)
    key_wg, key_wu, key_wd = jax.random.split(jax.random.key(seed + 1), 3)
    expert_ids, route_counts = draw_routing(key_route)
    tokens = jax.random.normal(key_tok, (GROUP_ROWS, MODEL_DIM), jnp.float32).astype(jnp.bfloat16)
    gate_w = jax.nn.softmax(jax.random.normal(key_gate, (GROUP_ROWS, TOP_K), jnp.float32), axis=-1)
    w_gate = (jax.random.normal(key_wg, (NUM_EXPERTS, MODEL_DIM, FFN_DIM), jnp.float32) * MODEL_DIM ** -0.5).astype(jnp.bfloat16)
    w_up = (jax.random.normal(key_wu, (NUM_EXPERTS, MODEL_DIM, FFN_DIM), jnp.float32) * MODEL_DIM ** -0.5).astype(jnp.bfloat16)
    w_down = (jax.random.normal(key_wd, (NUM_EXPERTS, FFN_DIM, MODEL_DIM), jnp.float32) * FFN_DIM ** -0.5).astype(jnp.bfloat16)
    return {"tokens": tokens, "expert_ids": expert_ids, "gate_w": gate_w, "route_counts": route_counts, "w_gate": w_gate, "w_up": w_up, "w_down": w_down}


def reference(tokens, expert_ids, gate_w, route_counts, w_gate, w_up, w_down):
    expert_ar = jnp.arange(NUM_EXPERTS)
    flat_ids = expert_ids.reshape(GROUP_SIZE, TOKENS_DEV * TOP_K)
    onehot = (flat_ids[:, :, None] == expert_ar).astype(jnp.int32)
    before = jnp.cumsum(onehot, axis=1) - onehot
    slot_idx = jnp.sum(before * onehot, axis=2).reshape(GROUP_SIZE, TOKENS_DEV, TOP_K)
    row_limit = jnp.sum(onehot * route_counts[:, None, :], axis=2).reshape(GROUP_SIZE, TOKENS_DEV, TOP_K)
    kept_mask = slot_idx < row_limit
    ids_3d = expert_ids.reshape(GROUP_SIZE, TOKENS_DEV, TOP_K)
    gates_3d = gate_w.reshape(GROUP_SIZE, TOKENS_DEV, TOP_K)
    tok_3d = tokens.reshape(GROUP_SIZE, TOKENS_DEV, MODEL_DIM).astype(jnp.float32)
    slot_hit = slot_idx[:, None, :, :] == jnp.arange(CAPACITY)[None, :, None, None]

    def one_expert(acc_out, blk_args):
        expert_id, gate_mat, up_mat, down_mat = blk_args
        place_mask = slot_hit & ((ids_3d == expert_id) & kept_mask)[:, None, :, :]
        disp_mat = jnp.sum(place_mask.astype(jnp.float32), axis=3)
        comb_w = jnp.sum(jnp.where(place_mask, gates_3d[:, None, :, :], 0.0), axis=3)
        rows_in = jnp.einsum("gct,gtd->gcd", disp_mat, tok_3d).astype(jnp.bfloat16).reshape(GROUP_SIZE * CAPACITY, MODEL_DIM)
        act_a = jnp.dot(rows_in, gate_mat, preferred_element_type=jnp.float32)
        act_b = jnp.dot(rows_in, up_mat, preferred_element_type=jnp.float32)
        hidden = (jax.nn.silu(act_a) * act_b).astype(jnp.bfloat16)
        rows_out = jnp.dot(hidden, down_mat, preferred_element_type=jnp.float32).astype(jnp.bfloat16)
        rows_out = rows_out.reshape(GROUP_SIZE, CAPACITY, MODEL_DIM).astype(jnp.float32)
        return acc_out + jnp.einsum("gct,gcd->gtd", comb_w, rows_out), None

    summed = lax.scan(one_expert, tok_3d, (expert_ar, w_gate, w_up, w_down))[0]
    return summed.astype(jnp.bfloat16).reshape(GROUP_ROWS, MODEL_DIM)
```

```python
import functools

import jax
import jax.numpy as jnp
from jax import lax
from jax.experimental import pallas as pl
from jax.experimental.pallas import tpu as pltpu
from jax.sharding import PartitionSpec as P

N_CHUNKS = 4
N_COLS = 4
GU_SLOTS = 4
DN_SLOTS = 2
F_BLOCK = 512
BF = jnp.bfloat16
F32 = jnp.float32
PHASES = ((0, 0), (0, 2), (1, 2), (1, 0))


def kernel(
    tok_hbm, ids_ref, gate_ref, cnt_ref, wg_hbm, wu_hbm, wd_hbm, out_ref,
    tok, maps, comb, gates, rows_in, hid, acc, ysend, yrecv, gu, dn,
    s_own, s_gu, s_dn, xs_send, xs_recv, ps_send, ps_recv, rs_send, rs_recv, ms_send, ms_recv, ys_send, ys_recv,
):
    tok_n, dim = tok_hbm.shape
    cap = tok_n // 2
    ffn = wg_hbm.shape[2]
    n_gu = ffn // F_BLOCK
    n_phase = len(PHASES)
    chunk = tok_n // N_CHUNKS
    cw = dim // N_COLS

    me = lax.axis_index("ep")
    core = me % 2
    partner = me + 1 - 2 * core
    devs = (me, partner, (me + 2) % 4, (partner + 2) % 4)

    def remote(src, dst, send, recv, peer):
        return pltpu.make_async_remote_copy(
            src_ref=src, dst_ref=dst, send_sem=send, recv_sem=recv,
            device_id={"ep": devs[peer]}, device_id_type=pl.DeviceIdType.MESH,
        )

    def gu_copies(g):
        phase = g // n_gu
        cols = pl.ds(pl.multiple_of((g % n_gu) * F_BLOCK, F_BLOCK), F_BLOCK)
        slot = g % GU_SLOTS
        exp = phase // 2
        return (
            pltpu.make_async_copy(wg_hbm.at[exp, :, cols], gu.at[slot, 0], s_gu.at[slot, 0]),
            pltpu.make_async_copy(wu_hbm.at[exp, :, cols], gu.at[slot, 1], s_gu.at[slot, 1]),
        )

    def gu_start(g):
        for c in gu_copies(g):
            c.start()

    def dn_copy(d):
        exp = (d // N_COLS) // 2
        cols = pl.ds((d % N_COLS) * cw, cw)
        return pltpu.make_async_copy(wd_hbm.at[exp, :, cols], dn.at[d % DN_SLOTS], s_dn.at[d % DN_SLOTS])

    own_copy = pltpu.make_async_copy(tok_hbm, tok.at[0], s_own)
    own_copy.start()
    for g in range(GU_SLOTS - 1):
        gu_start(g)
    for d in range(DN_SLOTS):
        dn_copy(d).start()

    barrier = pltpu.get_barrier_semaphore()
    for peer in (1, 2, 3):
        pl.semaphore_signal(barrier, inc=1, device_id={"ep": devs[peer]}, device_id_type=pl.DeviceIdType.MESH)
    pl.semaphore_wait(barrier, 3)

    def rows_of(c):
        return pl.ds(c * chunk, chunk)

    x_copies = [remote(tok_hbm.at[rows_of(c)], tok.at[2, rows_of(c)], xs_send.at[c], xs_recv.at[c], 2) for c in range(N_CHUNKS)]
    r_copies = [remote(tok.at[2, rows_of(c)], tok.at[3, rows_of(c)], rs_send.at[c], rs_recv.at[c], 1) for c in range(N_CHUNKS)]
    p_copy = remote(tok_hbm, tok.at[1], ps_send, ps_recv, 1)
    x_copies[0].start()
    p_copy.start()
    for c in range(1, N_CHUNKS):
        x_copies[c].start()

    row = lax.broadcasted_iota(jnp.int32, (8, 1), 0)
    exp_row = row % 2 + 2 * jnp.where(row < 2, devs[0], jnp.where(row < 4, devs[1], jnp.where(row < 6, devs[2], devs[3])))
    hit0 = ids_ref[0:1, :] == exp_row
    hit1 = ids_ref[1:2, :] == exp_row
    hit = jnp.where(hit0 | hit1, 1.0, 0.0)
    earlier = jnp.where(
        lax.broadcasted_iota(jnp.int32, (tok_n, tok_n), 0) < lax.broadcasted_iota(jnp.int32, (tok_n, tok_n), 1), 1.0, 0.0
    ).astype(BF)
    slot = jnp.dot(hit.astype(BF), earlier, preferred_element_type=F32)
    limit = jnp.sum(jnp.where(exp_row == lax.broadcasted_iota(jnp.int32, (8, 8), 1), cnt_ref[...], 0), axis=1, keepdims=True)
    served = (hit > 0.0) & (slot < limit.astype(F32))
    slot1 = jnp.where(served, slot + 1.0, 0.0)
    maps[0] = slot1
    gate_rows = jnp.where(hit0, gate_ref[0:1, :], 0.0) + jnp.where(hit1, gate_ref[1:2, :], 0.0)
    gates[...] = jnp.where(served, gate_rows, 0.0).T
    slot1_t = slot1.T
    lane = lax.broadcasted_iota(jnp.int32, (tok_n, cap), 1).astype(F32) + 1.0
    for i in range(8):
        comb[i] = jnp.where(slot1_t[:, i : i + 1] == lane, 1.0, 0.0).astype(BF)
    m_copies = [remote(maps.at[0], maps.at[r], ms_send.at[r - 1], ms_recv.at[r - 1], r) for r in (1, 2, 3)]
    for c in m_copies:
        c.start()

    own_copy.wait()
    for k in range(N_COLS):
        cols = pl.ds(k * cw, cw)
        acc[:, cols] = tok[0, :, cols].astype(F32)

    def gather(phase):
        exp, first = PHASES[phase]
        for half in range(2):
            peer = first + half
            if peer > 0 and exp == 0:
                m_copies[peer - 1].wait_recv()
            if peer == 1 and exp == 0:
                p_copy.wait_recv()
            if peer == 3 and exp == 0:
                for c in r_copies:
                    c.wait_recv()
            slots = lax.broadcasted_iota(jnp.int32, (cap, tok_n), 0).astype(F32) + 1.0
            pick = jnp.where(maps[peer, 2 * peer + exp : 2 * peer + exp + 1, :] == slots, 1.0, 0.0).astype(BF)
            for k in range(N_COLS):
                cols = pl.ds(k * cw, cw)
                got = jnp.dot(pick, tok[peer, :, cols], preferred_element_type=F32)
                rows_in[half * cap : (half + 1) * cap, cols] = got.astype(BF)

    def relay(c):
        x_copies[c].wait_recv()
        r_copies[c].start()

    def gate_up(phase):
        def step(s, carry):
            g = phase * n_gu + s
            for c in gu_copies(g):
                c.wait()

            @pl.when(g + GU_SLOTS - 1 < n_phase * n_gu)
            def _():
                gu_start(g + GU_SLOTS - 1)

            sl = g % GU_SLOTS
            a = jnp.dot(rows_in[...], gu[sl, 0], preferred_element_type=F32)
            b = jnp.dot(rows_in[...], gu[sl, 1], preferred_element_type=F32)
            h = (a * jax.nn.sigmoid(a) * b).astype(BF)
            hid[:, pl.ds(pl.multiple_of(s * F_BLOCK, F_BLOCK), F_BLOCK)] = h

            if phase == 0:
                @pl.when(s == n_gu // 2)
                def _():
                    relay(0)
            return carry

        lax.fori_loop(0, n_gu, step, 0)

    def y_copy(phase, k, half):
        exp, first = PHASES[phase]
        peer = first + half
        return remote(ysend.at[exp, peer, k], yrecv.at[exp, peer, k], ys_send.at[exp, peer, k], ys_recv.at[exp, peer, k], peer)

    def fold(exp, peer, k):
        i = 2 * peer + exp
        cols = pl.ds(k * cw, cw)
        src = ysend if peer == 0 else yrecv
        picked = jnp.dot(comb[i], src[exp, peer, k], preferred_element_type=F32)
        acc[:, cols] += gates[:, i : i + 1] * picked

    def wait_y(exp, peer, k):
        phase = PHASES.index((exp, 0 if peer < 2 else 2))
        y_copy(phase, k, peer % 2).wait_recv()

    def down_step(phase, k):
        exp, first = PHASES[phase]
        d = phase * N_COLS + k
        dn_copy(d).wait()
        y = jnp.dot(hid[...], dn[d % DN_SLOTS], preferred_element_type=F32).astype(BF)
        ysend[exp, first, k] = y[:cap]
        ysend[exp, first + 1, k] = y[cap:]
        if d + DN_SLOTS < n_phase * N_COLS:
            dn_copy(d + DN_SLOTS).start()
        for half in range(2):
            if first + half > 0:
                y_copy(phase, k, half).start()

    def finish(k):
        for peer in (2, 3, 1):
            wait_y(1, peer, k)
            fold(1, peer, k)
        fold(1, 0, k)
        cols = pl.ds(k * cw, cw)
        out_ref[:, cols] = acc[:, cols].astype(BF)

    gather(0)
    gate_up(0)
    relay(1)
    for k in range(N_COLS):
        down_step(0, k)
        if k == N_COLS // 2 - 1:
            relay(2)
    relay(3)
    gather(1)
    gate_up(1)
    for k in range(N_COLS):
        down_step(1, k)
        wait_y(0, 1, k)
        fold(0, 1, k)
        fold(0, 0, k)
    gather(2)
    gate_up(2)
    for k in range(N_COLS):
        down_step(2, k)
    gather(3)
    gate_up(3)
    for k in range(N_COLS):
        for peer in (2, 3):
            wait_y(0, peer, k)
            fold(0, peer, k)
    for k in range(N_COLS):
        down_step(3, k)
        if k > 0:
            finish(k - 1)
    finish(N_COLS - 1)

    for c in x_copies + r_copies + m_copies + [p_copy]:
        c.wait_send()
    for phase, (exp, first) in enumerate(PHASES):
        for k in range(N_COLS):
            for half in range(2):
                if first + half > 0:
                    y_copy(phase, k, half).wait_send()


def solution(mesh):
    row_spec = P(("dp", "ep"))

    def local_step(tokens, expert_ids, gate_w, route_counts, w_gate, w_up, w_down):
        tok_n, dim = tokens.shape
        ffn = w_gate.shape[2]
        cap = tok_n // 2
        cw = dim // N_COLS
        vmem = pl.BlockSpec(memory_space=pltpu.VMEM)
        hbm = pl.BlockSpec(memory_space=pl.ANY)
        dma = pltpu.SemaphoreType.DMA
        return pl.pallas_call(
            kernel,
            name="moe",
            out_shape=jax.ShapeDtypeStruct((tok_n, dim), BF),
            in_specs=[hbm, vmem, vmem, vmem, hbm, hbm, hbm],
            out_specs=vmem,
            scratch_shapes=[
                pltpu.VMEM((4, tok_n, dim), BF),
                pltpu.VMEM((4, 8, tok_n), F32),
                pltpu.VMEM((8, tok_n, cap), BF),
                pltpu.VMEM((tok_n, 8), F32),
                pltpu.VMEM((2 * cap, dim), BF),
                pltpu.VMEM((2 * cap, ffn), BF),
                pltpu.VMEM((tok_n, dim), F32),
                pltpu.VMEM((2, 4, N_COLS, cap, cw), BF),
                pltpu.VMEM((2, 4, N_COLS, cap, cw), BF),
                pltpu.VMEM((GU_SLOTS, 2, dim, F_BLOCK), BF),
                pltpu.VMEM((DN_SLOTS, ffn, cw), BF),
                dma, dma((GU_SLOTS, 2)), dma((DN_SLOTS,)),
                dma((N_CHUNKS,)), dma((N_CHUNKS,)), dma, dma,
                dma((N_CHUNKS,)), dma((N_CHUNKS,)), dma((3,)), dma((3,)),
                dma((2, 4, N_COLS)), dma((2, 4, N_COLS)),
            ],
            compiler_params=pltpu.CompilerParams(
                collective_id=0, has_side_effects=True, vmem_limit_bytes=66_000_000
            ),
        )(tokens, expert_ids.T, gate_w.T, route_counts, w_gate, w_up, w_down)

    return jax.shard_map(local_step, mesh=mesh, in_specs=(row_spec, row_spec, row_spec, row_spec, P("ep"), P("ep"), P("ep")), out_specs=row_spec, check_vma=False)
```

```python
import functools

import jax
import jax.numpy as jnp
from jax import lax
from jax.experimental import pallas as pl
from jax.experimental.pallas import tpu as pltpu
from jax.sharding import PartitionSpec as P

N_CHUNKS = 4
N_COLS = 4
GU_SLOTS = 8
GU_AHEAD = 3
DN_SLOTS = 2
F_BLOCK = 512
BF = jnp.bfloat16
F32 = jnp.float32
PHASES = ((0, 0), (0, 2), (1, 2), (1, 0))


def kernel(
    tok_hbm, ids_ref, gate_ref, cnt_ref, wg_hbm, wu_hbm, wd_hbm, out_ref,
    tok, maps, comb, gates, rows_in, hid, acc, ysend, yrecv, gu, dn,
    s_own, s_gu, s_dn, xs_send, xs_recv, ps_send, ps_recv, rs_send, rs_recv, ms_send, ms_recv, ys_send, ys_recv,
):
    tok_n, dim = tok_hbm.shape
    cap = tok_n // 2
    ffn = wg_hbm.shape[2]
    n_gu = ffn // F_BLOCK
    n_phase = len(PHASES)
    chunk = tok_n // N_CHUNKS
    cw = dim // N_COLS

    me = lax.axis_index("ep")
    core = me % 2
    partner = me + 1 - 2 * core
    devs = (me, partner, (me + 2) % 4, (partner + 2) % 4)

    def remote(src, dst, send, recv, peer):
        return pltpu.make_async_remote_copy(
            src_ref=src, dst_ref=dst, send_sem=send, recv_sem=recv,
            device_id={"ep": devs[peer]}, device_id_type=pl.DeviceIdType.MESH,
        )

    def gu_slot(exp, blk):
        return blk % GU_SLOTS if exp == 0 else (GU_SLOTS - 1 + n_gu * GU_SLOTS - blk) % GU_SLOTS

    def gu_copies(exp, blk):
        cols = pl.ds(pl.multiple_of(blk * F_BLOCK, F_BLOCK), F_BLOCK)
        slot = gu_slot(exp, blk)
        return (
            pltpu.make_async_copy(wg_hbm.at[exp, :, cols], gu.at[slot, 0], s_gu.at[slot, 0]),
            pltpu.make_async_copy(wu_hbm.at[exp, :, cols], gu.at[slot, 1], s_gu.at[slot, 1]),
        )

    def gu_start(exp, blk):
        for c in gu_copies(exp, blk):
            c.start()

    def dn_slot(exp, blk):
        return (blk + exp) % DN_SLOTS

    def dn_copy(exp, blk):
        slot = dn_slot(exp, blk)
        return pltpu.make_async_copy(wd_hbm.at[exp, :, pl.ds(blk * cw, cw)], dn.at[slot], s_dn.at[slot])

    own_copy = pltpu.make_async_copy(tok_hbm, tok.at[0], s_own)
    own_copy.start()
    for g in range(GU_AHEAD):
        gu_start(0, g)

    barrier = pltpu.get_barrier_semaphore()
    for peer in (1, 2, 3):
        pl.semaphore_signal(barrier, inc=1, device_id={"ep": devs[peer]}, device_id_type=pl.DeviceIdType.MESH)
    pl.semaphore_wait(barrier, 3)

    def rows_of(c):
        return pl.ds(c * chunk, chunk)

    x_copies = [remote(tok_hbm.at[rows_of(c)], tok.at[2, rows_of(c)], xs_send.at[c], xs_recv.at[c], 2) for c in range(N_CHUNKS)]
    r_copies = [remote(tok.at[2, rows_of(c)], tok.at[3, rows_of(c)], rs_send.at[c], rs_recv.at[c], 1) for c in range(N_CHUNKS)]
    p_copy = remote(tok_hbm, tok.at[1], ps_send, ps_recv, 1)
    x_copies[0].start()
    p_copy.start()
    for c in range(1, N_CHUNKS):
        x_copies[c].start()

    row = lax.broadcasted_iota(jnp.int32, (8, 1), 0)
    exp_row = row % 2 + 2 * jnp.where(row < 2, devs[0], jnp.where(row < 4, devs[1], jnp.where(row < 6, devs[2], devs[3])))
    hit0 = ids_ref[0:1, :] == exp_row
    hit1 = ids_ref[1:2, :] == exp_row
    hit = jnp.where(hit0 | hit1, 1.0, 0.0)
    earlier = jnp.where(
        lax.broadcasted_iota(jnp.int32, (tok_n, tok_n), 0) < lax.broadcasted_iota(jnp.int32, (tok_n, tok_n), 1), 1.0, 0.0
    ).astype(BF)
    slot = jnp.dot(hit.astype(BF), earlier, preferred_element_type=F32)
    limit = jnp.sum(jnp.where(exp_row == lax.broadcasted_iota(jnp.int32, (8, 8), 1), cnt_ref[...], 0), axis=1, keepdims=True)
    served = (hit > 0.0) & (slot < limit.astype(F32))
    slot1 = jnp.where(served, slot + 1.0, 0.0)
    maps[0] = slot1
    gate_rows = jnp.where(hit0, gate_ref[0:1, :], 0.0) + jnp.where(hit1, gate_ref[1:2, :], 0.0)
    gates[...] = jnp.where(served, gate_rows, 0.0).T
    slot1_t = slot1.T
    lane = lax.broadcasted_iota(jnp.int32, (tok_n, cap), 1).astype(F32) + 1.0
    for i in range(8):
        comb[i] = jnp.where(slot1_t[:, i : i + 1] == lane, 1.0, 0.0).astype(BF)
    m_copies = [remote(maps.at[0], maps.at[r], ms_send.at[r - 1], ms_recv.at[r - 1], r) for r in (1, 2, 3)]
    for c in m_copies:
        c.start()

    own_copy.wait()
    for k in range(N_COLS):
        cols = pl.ds(k * cw, cw)
        acc[:, cols] = tok[0, :, cols].astype(F32)

    def gather(phase):
        exp, first = PHASES[phase]
        for half in range(2):
            peer = first + half
            if peer > 0 and exp == 0:
                m_copies[peer - 1].wait_recv()
            if peer == 1 and exp == 0:
                p_copy.wait_recv()
            if peer == 3 and exp == 0:
                for c in r_copies:
                    c.wait_recv()
            slots = lax.broadcasted_iota(jnp.int32, (cap, tok_n), 0).astype(F32) + 1.0
            pick = jnp.where(maps[peer, 2 * peer + exp : 2 * peer + exp + 1, :] == slots, 1.0, 0.0).astype(BF)
            for k in range(N_COLS):
                cols = pl.ds(k * cw, cw)
                got = jnp.dot(pick, tok[peer, :, cols], preferred_element_type=F32)
                rows_in[half * cap : (half + 1) * cap, cols] = got.astype(BF)

    def relay(c):
        x_copies[c].wait_recv()
        r_copies[c].start()

    def gate_up(phase):
        exp = PHASES[phase][0]
        n_held = n_gu - GU_SLOTS

        def step(s, carry):
            if phase % 2 == 0:
                blk = s
                for c in gu_copies(exp, blk):
                    c.wait()
            else:
                blk = n_gu - 1 - s

                @pl.when(blk < n_held)
                def _():
                    for c in gu_copies(exp, blk):
                        c.wait()

            if phase == 0:
                @pl.when(s + GU_AHEAD < n_gu)
                def _():
                    gu_start(0, s + GU_AHEAD)

                for k in range(DN_SLOTS):
                    @pl.when(s == n_gu - 5 + 2 * k)
                    def _():
                        dn_copy(0, k).start()

                @pl.when(s == n_gu // 2)
                def _():
                    relay(0)
            else:
                if phase == 2:
                    @pl.when((s >= 1) & (s + GU_SLOTS - 1 < n_gu))
                    def _():
                        gu_start(1, s + GU_SLOTS - 1)
                else:
                    @pl.when((s >= 1) & (s <= n_held))
                    def _():
                        gu_start(exp, n_held - s)

                    if phase == 1:
                        @pl.when(s > n_held)
                        def _():
                            gu_start(1, s - n_held - 1)

            sl = gu_slot(exp, blk)
            a = jnp.dot(rows_in[...], gu[sl, 0], preferred_element_type=F32)
            b = jnp.dot(rows_in[...], gu[sl, 1], preferred_element_type=F32)
            h = (a * jax.nn.sigmoid(a) * b).astype(BF)
            hid[:, pl.ds(pl.multiple_of(blk * F_BLOCK, F_BLOCK), F_BLOCK)] = h
            return carry

        lax.fori_loop(0, n_gu, step, 0)
        if phase == 1:
            gu_start(1, GU_SLOTS - 1)

    def y_copy(phase, k, half):
        exp, first = PHASES[phase]
        peer = first + half
        return remote(ysend.at[exp, peer, k], yrecv.at[exp, peer - 1, k], ys_send.at[exp, peer, k], ys_recv.at[exp, peer, k], peer)

    def fold(exp, peer, k):
        i = 2 * peer + exp
        cols = pl.ds(k * cw, cw)
        rows = ysend[exp, 0, k] if peer == 0 else yrecv[exp, peer - 1, k]
        picked = jnp.dot(comb[i], rows, preferred_element_type=F32)
        acc[:, cols] += gates[:, i : i + 1] * picked

    def wait_y(exp, peer, k):
        phase = PHASES.index((exp, 0 if peer < 2 else 2))
        y_copy(phase, k, peer % 2).wait_recv()

    def down_step(phase, k):
        exp, first = PHASES[phase]
        step = k if phase % 2 == 0 else N_COLS - 1 - k
        if phase % 2 == 0 or step >= DN_SLOTS:
            dn_copy(exp, k).wait()
        y = jnp.dot(hid[...], dn[dn_slot(exp, k)], preferred_element_type=F32).astype(BF)
        ysend[exp, first, k] = y[:cap]
        ysend[exp, first + 1, k] = y[cap:]
        if phase % 2 == 0 and step + DN_SLOTS < N_COLS:
            dn_copy(exp, k + DN_SLOTS).start()
        if phase % 2 == 1 and step < N_COLS - DN_SLOTS:
            dn_copy(exp, N_COLS - DN_SLOTS - 1 - step).start()
        if phase == 1 and step >= N_COLS - DN_SLOTS:
            dn_copy(1, step - (N_COLS - DN_SLOTS)).start()
        for half in range(2):
            if first + half > 0:
                y_copy(phase, k, half).start()

    def finish(k):
        for peer in (2, 3, 1):
            wait_y(1, peer, k)
            fold(1, peer, k)
        fold(1, 0, k)
        cols = pl.ds(k * cw, cw)
        out_ref[:, cols] = acc[:, cols].astype(BF)

    gather(0)
    gate_up(0)
    relay(1)
    for k in range(N_COLS):
        down_step(0, k)
        if k == N_COLS // 2 - 1:
            relay(2)
    relay(3)
    gather(1)
    gate_up(1)
    for k in reversed(range(N_COLS)):
        down_step(1, k)
        wait_y(0, 1, k)
        fold(0, 1, k)
        fold(0, 0, k)
    gather(2)
    gate_up(2)
    for k in range(N_COLS):
        down_step(2, k)
    gather(3)
    gate_up(3)
    for k in range(N_COLS):
        for peer in (2, 3):
            wait_y(0, peer, k)
            fold(0, peer, k)
    for k in reversed(range(N_COLS)):
        down_step(3, k)
        if k < N_COLS - 1:
            finish(k + 1)
    finish(0)

    for c in x_copies + r_copies + m_copies + [p_copy]:
        c.wait_send()
    for phase, (exp, first) in enumerate(PHASES):
        for k in range(N_COLS):
            for half in range(2):
                if first + half > 0:
                    y_copy(phase, k, half).wait_send()


def solution(mesh):
    row_spec = P(("dp", "ep"))

    def local_step(tokens, expert_ids, gate_w, route_counts, w_gate, w_up, w_down):
        tok_n, dim = tokens.shape
        ffn = w_gate.shape[2]
        cap = tok_n // 2
        cw = dim // N_COLS
        vmem = pl.BlockSpec(memory_space=pltpu.VMEM)
        hbm = pl.BlockSpec(memory_space=pl.ANY)
        dma = pltpu.SemaphoreType.DMA
        return pl.pallas_call(
            kernel,
            name="moe",
            out_shape=jax.ShapeDtypeStruct((tok_n, dim), BF),
            in_specs=[hbm, vmem, vmem, vmem, hbm, hbm, hbm],
            out_specs=vmem,
            scratch_shapes=[
                pltpu.VMEM((4, tok_n, dim), BF),
                pltpu.VMEM((4, 8, tok_n), F32),
                pltpu.VMEM((8, tok_n, cap), BF),
                pltpu.VMEM((tok_n, 8), F32),
                pltpu.VMEM((2 * cap, dim), BF),
                pltpu.VMEM((2 * cap, ffn), BF),
                pltpu.VMEM((tok_n, dim), F32),
                pltpu.VMEM((2, 4, N_COLS, cap, cw), BF),
                pltpu.VMEM((2, 3, N_COLS, cap, cw), BF),
                pltpu.VMEM((GU_SLOTS, 2, dim, F_BLOCK), BF),
                pltpu.VMEM((DN_SLOTS, ffn, cw), BF),
                dma, dma((GU_SLOTS, 2)), dma((DN_SLOTS,)),
                dma((N_CHUNKS,)), dma((N_CHUNKS,)), dma, dma,
                dma((N_CHUNKS,)), dma((N_CHUNKS,)), dma((3,)), dma((3,)),
                dma((2, 4, N_COLS)), dma((2, 4, N_COLS)),
            ],
            compiler_params=pltpu.CompilerParams(
                collective_id=0, has_side_effects=True, vmem_limit_bytes=67_000_000
            ),
        )(tokens, expert_ids.T, gate_w.T, route_counts, w_gate, w_up, w_down)

    return jax.shard_map(local_step, mesh=mesh, in_specs=(row_spec, row_spec, row_spec, row_spec, P("ep"), P("ep"), P("ep")), out_specs=row_spec, check_vma=False)
```

```python
import jax
import jax.numpy as jnp
from jax import lax
from jax.experimental import pallas as pl
from jax.experimental.pallas import tpu as pltpu
from jax.sharding import PartitionSpec as P

N_CHUNKS = 4
N_COLS = 4
GU_SLOTS = 8
DN_SLOTS = 2
F_BLOCK = 512
GROUPS = ((0, 4), (4, 8), (8, 11))
BF = jnp.bfloat16
F32 = jnp.float32
N_PHASE = 4
FOLDS = ((1, 0), (0, 0), (0, 1), (1, 1))
SENT = 8
ZERO = 14


def kernel(
    tok_hbm, ids_ref, gate_ref, cnt_ref, wg_hbm, wu_hbm, wd_hbm, out_hbm,
    tok, maps, comb, gates, rows_in, hid, acc, ybuf, gu, dn,
    s_own, s_gu, s_dn, xs_send, xs_recv, ps_send, ps_recv, rs_send, rs_recv, ms_send, ms_recv, ys_send, ys_recv, s_out,
):
    tok_n, dim = tok_hbm.shape
    cap = tok_n // 2
    ffn = wg_hbm.shape[2]
    n_gu = ffn // F_BLOCK
    chunk = tok_n // N_CHUNKS
    cw = dim // N_COLS

    me = lax.axis_index("ep")
    partner = me + 1 - 2 * (me % 2)
    across = (me + 2) % 4
    diagonal = (partner + 2) % 4
    devs = (me, partner, across, diagonal)

    def remote(src, dst, send, recv, dev):
        return pltpu.make_async_remote_copy(
            src_ref=src, dst_ref=dst, send_sem=send, recv_sem=recv,
            device_id={"ep": dev}, device_id_type=pl.DeviceIdType.MESH,
        )

    def gu_slot(exp, blk):
        return jnp.where(exp == 0, blk % GU_SLOTS, (GU_SLOTS - 1 + n_gu * GU_SLOTS - blk) % GU_SLOTS)

    def gu_copies(exp, blk):
        cols = pl.ds(pl.multiple_of(blk * F_BLOCK, F_BLOCK), F_BLOCK)
        slot = gu_slot(exp, blk)
        return (
            pltpu.make_async_copy(wg_hbm.at[exp, :, cols], gu.at[slot, 0], s_gu.at[slot, 0]),
            pltpu.make_async_copy(wu_hbm.at[exp, :, cols], gu.at[slot, 1], s_gu.at[slot, 1]),
        )

    def gu_start(exp, blks):
        for blk in blks:
            for c in gu_copies(exp, blk):
                c.start()

    def dn_copy(d):
        cols = pl.ds(pl.multiple_of((d % N_COLS) * cw, cw), cw)
        slot = d % DN_SLOTS
        return pltpu.make_async_copy(wd_hbm.at[d // N_COLS // 2, :, cols], dn.at[slot], s_dn.at[slot])

    own_copy = pltpu.make_async_copy(tok_hbm, tok.at[0], s_own)
    own_copy.start()
    gu_start(0, range(4))

    barrier = pltpu.get_barrier_semaphore()
    for peer in (1, 2, 3):
        pl.semaphore_signal(barrier, inc=1, device_id={"ep": devs[peer]}, device_id_type=pl.DeviceIdType.MESH)
    pl.semaphore_wait(barrier, 3)

    def rows_of(c):
        return pl.ds(c * chunk, chunk)

    x_copies = [remote(tok_hbm.at[rows_of(c)], tok.at[2, rows_of(c)], xs_send.at[c], xs_recv.at[c], across) for c in range(N_CHUNKS)]
    r_copies = [remote(tok.at[2, rows_of(c)], tok.at[3, rows_of(c)], rs_send.at[c], rs_recv.at[c], partner) for c in range(N_CHUNKS)]
    p_copy = remote(tok_hbm, tok.at[1], ps_send, ps_recv, partner)
    x_copies[0].start()
    p_copy.start()
    for c in range(1, N_CHUNKS):
        x_copies[c].start()

    row = lax.broadcasted_iota(jnp.int32, (8, 1), 0)
    exp_row = row % 2 + 2 * jnp.where(row < 2, devs[0], jnp.where(row < 4, devs[1], jnp.where(row < 6, devs[2], devs[3])))
    hit0 = ids_ref[0:1, :] == exp_row
    hit1 = ids_ref[1:2, :] == exp_row
    hit = jnp.where(hit0 | hit1, 1.0, 0.0)
    earlier = jnp.where(
        lax.broadcasted_iota(jnp.int32, (tok_n, tok_n), 0) < lax.broadcasted_iota(jnp.int32, (tok_n, tok_n), 1), 1.0, 0.0
    ).astype(BF)
    slot = jnp.dot(hit.astype(BF), earlier, preferred_element_type=F32)
    limit = jnp.sum(jnp.where(exp_row == lax.broadcasted_iota(jnp.int32, (8, 8), 1), cnt_ref[...], 0), axis=1, keepdims=True)
    served = (hit > 0.0) & (slot < limit.astype(F32))
    slot1 = jnp.where(served, slot + 1.0, 0.0)
    maps[0] = slot1
    m_copies = [remote(maps.at[0], maps.at[r], ms_send.at[r - 1], ms_recv.at[r - 1], devs[r]) for r in (1, 2, 3)]
    for c in m_copies:
        c.start()
    gates_t = (jnp.where(hit0, gate_ref[0:1, :], 0.0) + jnp.where(hit1, gate_ref[1:2, :], 0.0)).T
    slot1_t = slot1.T
    lane = lax.broadcasted_iota(jnp.int32, (tok_n, cap), 1).astype(F32) + 1.0
    for f, (exp, side) in enumerate(FOLDS):
        for half in range(2):
            i = 2 * (2 * side + half) + exp
            comb[f, half] = jnp.where(slot1_t[:, i : i + 1] == lane, 1.0, 0.0).astype(BF)
            gates[f, :, half : half + 1] = gates_t[:, i : i + 1]
    for k in range(N_COLS):
        ybuf[ZERO, k] = jnp.zeros((cap, cw), BF)

    own_copy.wait()
    for k in range(N_COLS):
        cols = pl.ds(k * cw, cw)
        acc[:, cols] = tok[0, :, cols].astype(F32)

    def relay(c):
        x_copies[c].wait_recv()
        r_copies[c].start()

    def y_copy(exp, peer, k, dev):
        return remote(
            ybuf.at[SENT + 3 * exp + peer - 1, k], ybuf.at[4 * exp + peer, k], ys_send.at[exp, peer, k], ys_recv.at[exp, peer, k], dev
        )

    def folded(f, srcs, k):
        total = acc[:, k * cw : (k + 1) * cw]
        for half in range(2):
            picked = jnp.dot(comb[f, half], ybuf[srcs[half], k], preferred_element_type=F32)
            total += gates[f, :, half : half + 1] * picked
        return total

    def phase_step(p, carry):
        exp = p // 2
        rev = p % 2
        side = ((p + 1) // 2) % 2
        base = jnp.where(side == 0, me, across)
        base_partner = jnp.where(side == 0, partner, diagonal)

        @pl.when(p == 0)
        def _():
            p_copy.wait_recv()
            m_copies[0].wait_recv()

        @pl.when(p == 1)
        def _():
            relay(N_CHUNKS - 1)
            m_copies[1].wait_recv()
            m_copies[2].wait_recv()
            for c in r_copies:
                c.wait_recv()

        @pl.when(p > 0)
        def _():
            dn_copy(p * N_COLS + 1).start()

        def blk_of(s):
            return s + rev * (n_gu - 1 - 2 * s)

        for n, (first, last) in enumerate(GROUPS):
            @pl.when((rev == 0) | (n == 2))
            def _():
                for s in range(first, last):
                    for c in gu_copies(exp, blk_of(s)):
                        c.wait()

            @pl.when(p == 0)
            def _():
                if n == 0:
                    gu_start(0, range(4, 8))
                elif n == 1:
                    gu_start(0, range(8, n_gu))
                    dn_copy(0).start()
                else:
                    dn_copy(1).start()
                    relay(0)

            if n == 1:
                @pl.when(p == 1)
                def _():
                    gu_start(0, (2, 1, 0))
                    gu_start(1, (0,))

                @pl.when(p == 2)
                def _():
                    gu_start(1, (8, 9, 10))

                @pl.when(p == 3)
                def _():
                    gu_start(1, (2, 1, 0))
            elif n == 2:
                @pl.when(p == 1)
                def _():
                    gu_start(1, (1, 2, 3, 4))

            if n == 0:
                for half in range(2):
                    peer = 2 * side + half
                    slots = lax.broadcasted_iota(jnp.int32, (cap, tok_n), 0).astype(F32) + 1.0
                    pick = jnp.where(maps[peer, pl.ds(2 * peer + exp, 1), :] == slots, 1.0, 0.0).astype(BF)
                    for k in range(N_COLS):
                        cols = slice(k * cw, (k + 1) * cw)
                        got = jnp.dot(pick, tok[peer, :, cols], preferred_element_type=F32)
                        rows_in[half * cap : (half + 1) * cap, cols] = got.astype(BF)

            for s in range(first, last):
                sl = gu_slot(exp, blk_of(s))
                a = jnp.dot(rows_in[...], gu[sl, 0], preferred_element_type=F32)
                b = jnp.dot(rows_in[...], gu[sl, 1], preferred_element_type=F32)
                hid[:, pl.ds(pl.multiple_of(blk_of(s) * F_BLOCK, F_BLOCK), F_BLOCK)] = (a * jax.nn.sigmoid(a) * b).astype(BF)

        f_exp = p // 3
        f_side = p // 2
        srcs = [jnp.where(p == 0, ZERO, 4 * f_exp + 2 * f_side + half) for half in range(2)]
        top = jnp.where(side == 0, 4 * exp, SENT + 3 * exp + 1)
        low = SENT + 3 * exp + 2 * side
        for k in range(N_COLS):
            d = p * N_COLS + k
            dn_copy(d).wait()

            @pl.when(p > 0)
            def _():
                y_copy(f_exp, 2 * f_side + 1, k, me).wait_recv()

            @pl.when(p > 1)
            def _():
                y_copy(f_exp, 2, k, me).wait_recv()

            if k > 0:
                @pl.when(d + 1 < N_PHASE * N_COLS)
                def _():
                    dn_copy(d + 1).start()
            else:
                @pl.when(p == 1)
                def _():
                    gu_start(1, (5, 6, 7))

            if k % 2 == 0:
                @pl.when(p == 0)
                def _():
                    relay(1 + k // 2)

            acc[:, k * cw : (k + 1) * cw] = folded(p, srcs, k)
            y = jnp.dot(hid[...], dn[d % DN_SLOTS], preferred_element_type=F32).astype(BF)
            ybuf[top, k] = y[:cap]
            ybuf[low, k] = y[cap:]
            y_copy(exp, 2 * side + 1, k, base_partner).start()

            @pl.when(side == 1)
            def _():
                y_copy(exp, 2, k, base).start()
        return carry

    lax.fori_loop(0, N_PHASE, phase_step, 0)

    outs = []
    for k in range(N_COLS):
        y_copy(1, 1, k, partner).wait_recv()
        cols = slice(k * cw, (k + 1) * cw)
        rows_in[:, cols] = folded(0, (4, 5), k).astype(BF)
        outs.append(pltpu.make_async_copy(rows_in.at[:, cols], out_hbm.at[:, cols], s_out.at[k]))
        outs[k].start()

    for c in x_copies + r_copies + m_copies + [p_copy]:
        c.wait_send()
    for exp in range(2):
        for peer in range(1, 4):
            for k in range(N_COLS):
                y_copy(exp, peer, k, devs[peer]).wait_send()
    for c in outs:
        c.wait()


def solution(mesh):
    row_spec = P(("dp", "ep"))

    def local_step(tokens, expert_ids, gate_w, route_counts, w_gate, w_up, w_down):
        tok_n, dim = tokens.shape
        ffn = w_gate.shape[2]
        cap = tok_n // 2
        cw = dim // N_COLS
        vmem = pl.BlockSpec(memory_space=pltpu.VMEM)
        hbm = pl.BlockSpec(memory_space=pl.ANY)
        dma = pltpu.SemaphoreType.DMA
        return pl.pallas_call(
            kernel,
            name="moe",
            out_shape=jax.ShapeDtypeStruct((tok_n, dim), BF),
            in_specs=[hbm, vmem, vmem, vmem, hbm, hbm, hbm],
            out_specs=hbm,
            scratch_shapes=[
                pltpu.VMEM((4, tok_n, dim), BF),
                pltpu.VMEM((4, 8, tok_n), F32),
                pltpu.VMEM((4, 2, tok_n, cap), BF),
                pltpu.VMEM((4, tok_n, 2), F32),
                pltpu.VMEM((2 * cap, dim), BF),
                pltpu.VMEM((2 * cap, ffn), BF),
                pltpu.VMEM((tok_n, dim), F32),
                pltpu.VMEM((ZERO + 1, N_COLS, cap, cw), BF),
                pltpu.VMEM((GU_SLOTS, 2, dim, F_BLOCK), BF),
                pltpu.VMEM((DN_SLOTS, ffn, cw), BF),
                dma, dma((GU_SLOTS, 2)), dma((DN_SLOTS,)),
                dma((N_CHUNKS,)), dma((N_CHUNKS,)), dma, dma,
                dma((N_CHUNKS,)), dma((N_CHUNKS,)), dma((3,)), dma((3,)),
                dma((2, 4, N_COLS)), dma((2, 4, N_COLS)), dma((N_COLS,)),
            ],
            compiler_params=pltpu.CompilerParams(
                collective_id=0, has_side_effects=True, vmem_limit_bytes=67_000_000
            ),
        )(tokens, expert_ids.T, gate_w.T, route_counts, w_gate, w_up, w_down)

    return jax.shard_map(local_step, mesh=mesh, in_specs=(row_spec, row_spec, row_spec, row_spec, P("ep"), P("ep"), P("ep")), out_specs=row_spec, check_vma=False)
```

```python
import jax
import jax.numpy as jnp
from jax import lax
from jax.experimental import pallas as pl
from jax.experimental.pallas import tpu as pltpu
from jax.sharding import PartitionSpec as P

N_CHUNKS = 4
N_COLS = 4
GU_SLOTS = 8
DN_SLOTS = 6
F_BLOCK = 512
GROUPS = ((0, 4), (4, 8), (8, 11))
BF = jnp.bfloat16
F32 = jnp.float32
N_PHASE = 4
FOLDS = ((1, 0), (0, 0), (0, 1), (1, 1))
RECV = 8


def kernel(
    tok_hbm, ids_ref, gate_ref, cnt_ref, wg_hbm, wu_hbm, wd_hbm, out_hbm,
    buf, maps, gates, hid, acc, gu, dn,
    s_own, s_gu, s_dn, xs_send, xs_recv, ps_send, ps_recv, rs_send, rs_recv, ms_send, ms_recv, ys_send, ys_recv, s_out,
):
    _, cap, dim = tok_hbm.shape
    tok_n = 2 * cap
    ffn = wg_hbm.shape[2]
    n_gu = ffn // F_BLOCK
    chunk = tok_n // N_CHUNKS
    cw = dim // N_COLS
    hw = cw // 2

    me = lax.axis_index("ep")
    partner = me + 1 - 2 * (me % 2)
    across = (me + 2) % 4
    diagonal = (partner + 2) % 4
    devs = (me, partner, across, diagonal)

    def remote(src, dst, send, recv, dev):
        return pltpu.make_async_remote_copy(
            src_ref=src, dst_ref=dst, send_sem=send, recv_sem=recv,
            device_id={"ep": dev}, device_id_type=pl.DeviceIdType.MESH,
        )

    def gu_slot(exp, blk):
        return jnp.where(exp == 0, blk % GU_SLOTS, (GU_SLOTS - 1 + n_gu * GU_SLOTS - blk) % GU_SLOTS)

    def gu_copies(exp, blk):
        cols = pl.ds(pl.multiple_of(blk * F_BLOCK, F_BLOCK), F_BLOCK)
        slot = gu_slot(exp, blk)
        return (
            pltpu.make_async_copy(wg_hbm.at[exp, :, cols], gu.at[slot, 0], s_gu.at[slot, 0]),
            pltpu.make_async_copy(wu_hbm.at[exp, :, cols], gu.at[slot, 1], s_gu.at[slot, 1]),
        )

    def gu_start(exp, blks):
        for blk in blks:
            for c in gu_copies(exp, blk):
                c.start()

    def dn_copy(h):
        cols = pl.ds(pl.multiple_of((h % (2 * N_COLS)) * hw, hw), hw)
        slot = h % DN_SLOTS
        return pltpu.make_async_copy(wd_hbm.at[h // (4 * N_COLS), :, cols], dn.at[slot], s_dn.at[slot])

    def dn_start(h):
        dn_copy(h).start()
        dn_copy(h + 1).start()

    own_copy = pltpu.make_async_copy(tok_hbm, buf.at[pl.ds(0, 2)], s_own)
    own_copy.start()
    gu_start(0, range(4))

    barrier = pltpu.get_barrier_semaphore()
    for peer in (1, 2, 3):
        pl.semaphore_signal(barrier, inc=1, device_id={"ep": devs[peer]}, device_id_type=pl.DeviceIdType.MESH)
    pl.semaphore_wait(barrier, 3)

    def rows_of(peer, c):
        return buf.at[2 * peer + c // (N_CHUNKS // 2), pl.ds(c % (N_CHUNKS // 2) * chunk, chunk)]

    x_copies = [
        remote(tok_hbm.at[c // (N_CHUNKS // 2), pl.ds(c % (N_CHUNKS // 2) * chunk, chunk)], rows_of(2, c), xs_send.at[c], xs_recv.at[c], across)
        for c in range(N_CHUNKS)
    ]
    r_copies = [remote(rows_of(2, c), rows_of(3, c), rs_send.at[c], rs_recv.at[c], partner) for c in range(N_CHUNKS)]
    p_copy = remote(tok_hbm, buf.at[pl.ds(2, 2)], ps_send, ps_recv, partner)
    x_copies[0].start()
    p_copy.start()
    for c in range(1, N_CHUNKS):
        x_copies[c].start()

    row = lax.broadcasted_iota(jnp.int32, (8, 1), 0)
    exp_row = row % 2 + 2 * jnp.where(row < 2, devs[0], jnp.where(row < 4, devs[1], jnp.where(row < 6, devs[2], devs[3])))
    hit0 = ids_ref[0:1, :] == exp_row
    hit1 = ids_ref[1:2, :] == exp_row
    hit = jnp.where(hit0 | hit1, 1.0, 0.0)
    earlier = jnp.where(
        lax.broadcasted_iota(jnp.int32, (tok_n, tok_n), 0) < lax.broadcasted_iota(jnp.int32, (tok_n, tok_n), 1), 1.0, 0.0
    ).astype(BF)
    slot = jnp.dot(hit.astype(BF), earlier, preferred_element_type=F32)
    limit = jnp.sum(jnp.where(exp_row == lax.broadcasted_iota(jnp.int32, (8, 8), 1), cnt_ref[...], 0), axis=1, keepdims=True)
    served = (hit > 0.0) & (slot < limit.astype(F32))
    slot1 = jnp.where(served, slot + 1.0, 0.0)
    maps[0] = slot1
    m_copies = [remote(maps.at[0], maps.at[r], ms_send.at[r - 1], ms_recv.at[r - 1], devs[r]) for r in (1, 2, 3)]
    for c in m_copies:
        c.start()
    gates_t = (jnp.where(hit0, gate_ref[0:1, :], 0.0) + jnp.where(hit1, gate_ref[1:2, :], 0.0)).T
    slot1_t = slot1.T
    for f, (exp, side) in enumerate(FOLDS):
        for half in range(2):
            i = 2 * (2 * side + half) + exp
            gates[f, :, half : half + 1] = gates_t[:, i : i + 1]
            gates[f, :, 2 + half : 3 + half] = slot1_t[:, i : i + 1]
    own_copy.wait()
    for k in range(N_COLS):
        for half in range(2):
            acc[half * cap : (half + 1) * cap, k * cw : (k + 1) * cw] = buf[half, :, k * cw : (k + 1) * cw].astype(F32)

    def relay(c):
        x_copies[c].wait_recv()
        r_copies[c].start()

    def y_copy(exp, peer, part, k, dev):
        cols = pl.ds(k * cw, cw)
        return remote(buf.at[part, :, cols], buf.at[RECV + 3 * exp + peer - 1, :, cols], ys_send.at[exp, peer, k], ys_recv.at[exp, peer, k], dev)

    def folded(f, base_slot, srcs, k):
        total = acc[:, k * cw : (k + 1) * cw]
        lane = (lax.broadcasted_iota(jnp.int32, (tok_n, cap), 1) + base_slot).astype(F32)
        for half in range(2):
            comb = jnp.where(gates[f, :, 2 + half : 3 + half] == lane, 1.0, 0.0).astype(BF)
            picked = jnp.dot(comb, buf[srcs[half], :, k * cw : (k + 1) * cw], preferred_element_type=F32)
            total += gates[f, :, half : half + 1] * picked
        return total

    def gather(side):
        slots = lax.broadcasted_iota(jnp.int32, (cap, tok_n), 0).astype(F32) + 1.0
        picks = [
            [
                jnp.where(maps[2 * side + half, pl.ds(2 * (2 * side + half) + exp, 1), :] == slots, 1.0, 0.0).astype(BF)
                for half in range(2)
            ]
            for exp in range(2)
        ]
        for k in range(N_COLS):
            cols = slice(k * cw, (k + 1) * cw)
            toks = [buf[pl.ds(4 * side + 2 * half, 2), :, cols].reshape(tok_n, cw) for half in range(2)]
            got = [[jnp.dot(picks[exp][half], toks[half], preferred_element_type=F32).astype(BF) for half in range(2)] for exp in range(2)]
            for exp in range(2):
                for half in range(2):
                    buf[4 * side + 2 * (1 - exp) + half, :, cols] = got[exp][half]

    def phase_step(p, carry):
        exp = p // 2
        rev = p % 2
        side = ((p + 1) // 2) % 2
        base = jnp.where(side == 0, me, across)
        base_partner = jnp.where(side == 0, partner, diagonal)

        work = 4 * side + 2 * (1 - exp)

        @pl.when(p == 0)
        def _():
            p_copy.wait_recv()
            m_copies[0].wait_recv()

        @pl.when(p == 1)
        def _():
            m_copies[1].wait_recv()
            m_copies[2].wait_recv()
            for c in r_copies:
                c.wait_recv()
                c.wait_send()

        @pl.when(p < 2)
        def _():
            gather(side)

        def blk_of(s):
            return s + rev * (n_gu - 1 - 2 * s)

        for n, (first, last) in enumerate(GROUPS):
            @pl.when((rev == 0) | (n == 2))
            def _():
                for s in range(first, last):
                    for c in gu_copies(exp, blk_of(s)):
                        c.wait()

            @pl.when(p == 0)
            def _():
                if n == 0:
                    gu_start(0, range(4, 8))
                elif n == 1:
                    gu_start(0, range(8, n_gu))
                    dn_start(0)
                else:
                    dn_start(2)
                    relay(0)

            if n == 1:
                @pl.when(p == 1)
                def _():
                    gu_start(0, (2, 1, 0))
                    gu_start(1, (0,))

                @pl.when(p == 2)
                def _():
                    gu_start(1, (8, 9, 10))

                @pl.when(p == 3)
                def _():
                    gu_start(1, (2, 1, 0))
            elif n == 2:
                dn_start(p * 2 * N_COLS + 4)

                @pl.when(p == 1)
                def _():
                    gu_start(1, (1, 2, 3))

            rows = buf.at[pl.ds(work, 2)]
            for s in range(first, last):
                sl = gu_slot(exp, blk_of(s))
                a = jnp.dot(rows[...].reshape(tok_n, dim), gu[sl, 0], preferred_element_type=F32)
                b = jnp.dot(rows[...].reshape(tok_n, dim), gu[sl, 1], preferred_element_type=F32)
                hid[:, pl.ds(pl.multiple_of(blk_of(s) * F_BLOCK, F_BLOCK), F_BLOCK)] = (a * jax.nn.sigmoid(a) * b).astype(BF)

        f_exp = p // 3
        f_side = p // 2
        base_slot = jnp.where(p == 0, tok_n, 1)
        src0 = jnp.where(p == 0, 0, jnp.where(p == 1, 2, RECV + 3 * f_exp + 1))
        src1 = jnp.where(p == 0, 0, RECV + 3 * f_exp + 2 * f_side)
        for k in range(N_COLS):
            h = 2 * (p * N_COLS + k)
            for i in range(2):
                dn_copy(h + i).wait()

            @pl.when(p > 0)
            def _():
                y_copy(f_exp, 2 * f_side + 1, 0, k, me).wait_recv()

            @pl.when(p > 1)
            def _():
                y_copy(f_exp, 2, 0, k, me).wait_recv()

            if k > 0:
                @pl.when(h + 4 < 2 * N_PHASE * N_COLS)
                def _():
                    dn_start(h + 4)

            if k > 1:
                @pl.when(p == 1)
                def _():
                    gu_start(1, (2 * k, 2 * k + 1))

            if k != 1:
                @pl.when(p == 0)
                def _():
                    relay(max(k, 1))

            acc[:, k * cw : (k + 1) * cw] = folded(p, base_slot, (src0, src1), k)
            for i in range(2):
                y = jnp.dot(hid[...], dn[(h + i) % DN_SLOTS], preferred_element_type=F32).astype(BF)
                for half in range(2):
                    buf[work + half, :, k * cw + i * hw : k * cw + (i + 1) * hw] = y[half * cap : (half + 1) * cap]
            y_copy(exp, 2 * side + 1, work + 1, k, base_partner).start()

            @pl.when(side == 1)
            def _():
                y_copy(exp, 2, work, k, base).start()
        return carry

    lax.fori_loop(0, N_PHASE, phase_step, 0)

    for k in range(N_COLS):
        y_copy(0, 1, 3, k, partner).wait_send()
    outs = []
    for k in range(N_COLS):
        y_copy(1, 1, 1, k, partner).wait_recv()
        cols = slice(k * cw, (k + 1) * cw)
        total = folded(0, 1, (0, RECV + 3), k).astype(BF)
        for half in range(2):
            buf[2 + half, :, cols] = total[half * cap : (half + 1) * cap]
        outs.append(pltpu.make_async_copy(buf.at[pl.ds(2, 2), :, cols], out_hbm.at[:, :, cols], s_out.at[k]))
        outs[k].start()

    for c in x_copies + m_copies + [p_copy]:
        c.wait_send()
    for exp in range(2):
        for peer in range(1, 4):
            for k in range(N_COLS):
                if exp + peer > 1:
                    y_copy(exp, peer, 0, k, devs[peer]).wait_send()
    for c in outs:
        c.wait()


def solution(mesh):
    row_spec = P(("dp", "ep"))

    def local_step(tokens, expert_ids, gate_w, route_counts, w_gate, w_up, w_down):
        tok_n, dim = tokens.shape
        ffn = w_gate.shape[2]
        cap = tok_n // 2
        cw = dim // N_COLS
        vmem = pl.BlockSpec(memory_space=pltpu.VMEM)
        hbm = pl.BlockSpec(memory_space=pl.ANY)
        dma = pltpu.SemaphoreType.DMA
        return pl.pallas_call(
            kernel,
            name="moe",
            out_shape=jax.ShapeDtypeStruct((2, cap, dim), BF),
            in_specs=[hbm, vmem, vmem, vmem, hbm, hbm, hbm],
            out_specs=hbm,
            scratch_shapes=[
                pltpu.VMEM((RECV + 6, cap, dim), BF),
                pltpu.VMEM((4, 8, tok_n), F32),
                pltpu.VMEM((4, tok_n, 4), F32),
                pltpu.VMEM((2 * cap, ffn), BF),
                pltpu.VMEM((tok_n, dim), F32),
                pltpu.VMEM((GU_SLOTS, 2, dim, F_BLOCK), BF),
                pltpu.VMEM((DN_SLOTS, ffn, cw // 2), BF),
                dma, dma((GU_SLOTS, 2)), dma((DN_SLOTS,)),
                dma((N_CHUNKS,)), dma((N_CHUNKS,)), dma, dma,
                dma((N_CHUNKS,)), dma((N_CHUNKS,)), dma((3,)), dma((3,)),
                dma((2, 4, N_COLS)), dma((2, 4, N_COLS)), dma((N_COLS,)),
            ],
            compiler_params=pltpu.CompilerParams(
                collective_id=0, has_side_effects=True, vmem_limit_bytes=67_000_000
            ),
        )(tokens.reshape(2, cap, dim), expert_ids.T, gate_w.T, route_counts, w_gate, w_up, w_down).reshape(tok_n, dim)

    return jax.shard_map(local_step, mesh=mesh, in_specs=(row_spec, row_spec, row_spec, row_spec, P("ep"), P("ep"), P("ep")), out_specs=row_spec, check_vma=False)
```

```python
import jax
import jax.numpy as jnp
from jax import lax
from jax.experimental import pallas as pl
from jax.experimental.pallas import tpu as pltpu
from jax.sharding import PartitionSpec as P

N_CHUNKS = 4
N_COLS = 4
GU_SLOTS = 8
DN_SLOTS = 6
F_BLOCK = 512
GROUPS = ((0, 2), (2, 5), (5, 8), (8, 11))
BF = jnp.bfloat16
F32 = jnp.float32
N_PHASE = 4
FOLDS = ((1, 0), (0, 0), (0, 1), (1, 1))
RECV = 8


def kernel(
    tok_hbm, ids_ref, gate_ref, cnt_ref, wg_hbm, wu_hbm, wd_hbm, out_hbm,
    buf, maps, gates, hid, acc, gu, dn,
    s_own, s_gu, s_dn, xs_send, xs_recv, ps_send, ps_recv, rs_send, rs_recv, ms_send, ms_recv, ys_send, ys_recv, s_out,
):
    _, cap, dim = tok_hbm.shape
    tok_n = 2 * cap
    ffn = wg_hbm.shape[2]
    n_gu = ffn // F_BLOCK
    chunk = tok_n // N_CHUNKS
    cw = dim // N_COLS
    hw = cw // 2

    me = lax.axis_index("ep")
    partner = me + 1 - 2 * (me % 2)
    across = (me + 2) % 4
    diagonal = (partner + 2) % 4
    devs = (me, partner, across, diagonal)

    def remote(src, dst, send, recv, dev):
        return pltpu.make_async_remote_copy(
            src_ref=src, dst_ref=dst, send_sem=send, recv_sem=recv,
            device_id={"ep": dev}, device_id_type=pl.DeviceIdType.MESH,
        )

    def gu_slot(exp, blk):
        return jnp.where(exp == 0, blk % GU_SLOTS, (GU_SLOTS - 1 + n_gu * GU_SLOTS - blk) % GU_SLOTS)

    def gu_copies(exp, blk):
        cols = pl.ds(pl.multiple_of(blk * F_BLOCK, F_BLOCK), F_BLOCK)
        slot = gu_slot(exp, blk)
        return (
            pltpu.make_async_copy(wg_hbm.at[exp, :, cols], gu.at[slot, 0], s_gu.at[slot, 0]),
            pltpu.make_async_copy(wu_hbm.at[exp, :, cols], gu.at[slot, 1], s_gu.at[slot, 1]),
        )

    def gu_start(exp, blks):
        for blk in blks:
            for c in gu_copies(exp, blk):
                c.start()

    def dn_copy(h):
        cols = pl.ds(pl.multiple_of((h % (2 * N_COLS)) * hw, hw), hw)
        slot = h % DN_SLOTS
        return pltpu.make_async_copy(wd_hbm.at[h // (4 * N_COLS), :, cols], dn.at[slot], s_dn.at[slot])

    def dn_start(h):
        dn_copy(h).start()
        dn_copy(h + 1).start()

    own_copy = pltpu.make_async_copy(tok_hbm, buf.at[pl.ds(0, 2)], s_own)
    own_copy.start()
    gu_start(0, range(2))

    barrier = pltpu.get_barrier_semaphore()
    for peer in (1, 2, 3):
        pl.semaphore_signal(barrier, inc=1, device_id={"ep": devs[peer]}, device_id_type=pl.DeviceIdType.MESH)
    pl.semaphore_wait(barrier, 3)

    def rows_of(peer, c):
        return buf.at[2 * peer + c // (N_CHUNKS // 2), pl.ds(c % (N_CHUNKS // 2) * chunk, chunk)]

    x_copies = [
        remote(tok_hbm.at[c // (N_CHUNKS // 2), pl.ds(c % (N_CHUNKS // 2) * chunk, chunk)], rows_of(2, c), xs_send.at[c], xs_recv.at[c], across)
        for c in range(N_CHUNKS)
    ]
    r_copies = [remote(rows_of(2, c), rows_of(3, c), rs_send.at[c], rs_recv.at[c], partner) for c in range(N_CHUNKS)]
    p_copy = remote(tok_hbm, buf.at[pl.ds(2, 2)], ps_send, ps_recv, partner)
    x_copies[0].start()
    p_copy.start()
    for c in range(1, N_CHUNKS):
        x_copies[c].start()

    row = lax.broadcasted_iota(jnp.int32, (8, 1), 0)
    exp_row = row % 2 + 2 * jnp.where(row < 2, devs[0], jnp.where(row < 4, devs[1], jnp.where(row < 6, devs[2], devs[3])))
    hit0 = ids_ref[0:1, :] == exp_row
    hit1 = ids_ref[1:2, :] == exp_row
    hit = jnp.where(hit0 | hit1, 1.0, 0.0)
    earlier = jnp.where(
        lax.broadcasted_iota(jnp.int32, (tok_n, tok_n), 0) < lax.broadcasted_iota(jnp.int32, (tok_n, tok_n), 1), 1.0, 0.0
    ).astype(BF)
    slot = jnp.dot(hit.astype(BF), earlier, preferred_element_type=F32)
    limit = jnp.sum(jnp.where(exp_row == lax.broadcasted_iota(jnp.int32, (8, 8), 1), cnt_ref[...], 0), axis=1, keepdims=True)
    served = (hit > 0.0) & (slot < limit.astype(F32))
    slot1 = jnp.where(served, slot + 1.0, 0.0)
    maps[0] = slot1
    m_copies = [remote(maps.at[0], maps.at[r], ms_send.at[r - 1], ms_recv.at[r - 1], devs[r]) for r in (1, 2, 3)]
    for c in m_copies:
        c.start()
    gates_t = (jnp.where(hit0, gate_ref[0:1, :], 0.0) + jnp.where(hit1, gate_ref[1:2, :], 0.0)).T
    slot1_t = slot1.T
    for f, (exp, side) in enumerate(FOLDS):
        for half in range(2):
            i = 2 * (2 * side + half) + exp
            gates[f, :, half : half + 1] = gates_t[:, i : i + 1]
            gates[f, :, 2 + half : 3 + half] = slot1_t[:, i : i + 1]
    own_copy.wait()
    gu_start(0, range(2, 5))
    for k in range(N_COLS):
        for half in range(2):
            acc[half * cap : (half + 1) * cap, k * cw : (k + 1) * cw] = buf[half, :, k * cw : (k + 1) * cw].astype(F32)

    def relay(c):
        x_copies[c].wait_recv()
        r_copies[c].start()

    def y_copy(exp, peer, part, k, dev):
        cols = pl.ds(k * cw, cw)
        return remote(buf.at[part, :, cols], buf.at[RECV + 3 * exp + peer - 1, :, cols], ys_send.at[exp, peer, k], ys_recv.at[exp, peer, k], dev)

    def folded(f, base_slot, srcs, k, total=None):
        total = acc[:, k * cw : (k + 1) * cw] if total is None else total
        lane = (lax.broadcasted_iota(jnp.int32, (tok_n, cap), 1) + base_slot).astype(F32)
        for half in range(2):
            comb = jnp.where(gates[f, :, 2 + half : 3 + half] == lane, 1.0, 0.0).astype(BF)
            picked = jnp.dot(comb, buf[srcs[half], :, k * cw : (k + 1) * cw], preferred_element_type=F32)
            total += gates[f, :, half : half + 1] * picked
        return total

    def gather(side):
        slots = lax.broadcasted_iota(jnp.int32, (cap, tok_n), 0).astype(F32) + 1.0
        picks = [
            [
                jnp.where(maps[2 * side + half, pl.ds(2 * (2 * side + half) + exp, 1), :] == slots, 1.0, 0.0).astype(BF)
                for half in range(2)
            ]
            for exp in range(2)
        ]
        for k in range(N_COLS):
            cols = slice(k * cw, (k + 1) * cw)
            toks = [buf[pl.ds(4 * side + 2 * half, 2), :, cols].reshape(tok_n, cw) for half in range(2)]
            got = [[jnp.dot(picks[exp][half], toks[half], preferred_element_type=F32).astype(BF) for half in range(2)] for exp in range(2)]
            for exp in range(2):
                for half in range(2):
                    buf[4 * side + 2 * (1 - exp) + half, :, cols] = got[exp][half]

    def phase_step(p, carry):
        exp = p // 2
        rev = p % 2
        side = ((p + 1) // 2) % 2
        base = jnp.where(side == 0, me, across)
        base_partner = jnp.where(side == 0, partner, diagonal)

        work = 4 * side + 2 * (1 - exp)

        @pl.when(p == 0)
        def _():
            p_copy.wait_recv()
            m_copies[0].wait_recv()

        @pl.when(p == 1)
        def _():
            m_copies[1].wait_recv()
            m_copies[2].wait_recv()
            for c in r_copies:
                c.wait_recv()
                c.wait_send()

        @pl.when(p < 2)
        def _():
            gather(side)

        def blk_of(s):
            return s + rev * (n_gu - 1 - 2 * s)

        for n, (first, last) in enumerate(GROUPS):
            @pl.when((rev == 0) | (n == 3))
            def _():
                for s in range(first, last):
                    for c in gu_copies(exp, blk_of(s)):
                        c.wait()

            @pl.when(p == 0)
            def _():
                if n == 0:
                    gu_start(0, (5, 6, 7))
                elif n == 1:
                    gu_start(0, (8, 9))
                elif n == 2:
                    gu_start(0, (10,))
                    dn_start(0)
                else:
                    dn_start(2)
                    relay(0)

            @pl.when(p == 1)
            def _():
                if n == 1:
                    gu_start(0, (2, 1))
                elif n == 2:
                    gu_start(0, (0,))
                    gu_start(1, (0, 1))
                elif n == 3:
                    gu_start(1, (2, 3, 4))

            @pl.when(p == 2)
            def _():
                if n == 1:
                    gu_start(1, (8, 9))
                elif n == 2:
                    gu_start(1, (10,))

            @pl.when(p == 3)
            def _():
                if n == 1:
                    gu_start(1, (2, 1))
                elif n == 2:
                    gu_start(1, (0,))

            if n == 3:
                dn_start(p * 2 * N_COLS + 4)

            rows = buf.at[pl.ds(work, 2)]
            for s in range(first, last):
                sl = gu_slot(exp, blk_of(s))
                a = jnp.dot(rows[...].reshape(tok_n, dim), gu[sl, 0], preferred_element_type=F32)
                b = jnp.dot(rows[...].reshape(tok_n, dim), gu[sl, 1], preferred_element_type=F32)
                hid[:, pl.ds(pl.multiple_of(blk_of(s) * F_BLOCK, F_BLOCK), F_BLOCK)] = (a * jax.nn.sigmoid(a) * b).astype(BF)

        for k in range(N_COLS):
            h = 2 * (p * N_COLS + k)
            for i in range(2):
                dn_copy(h + i).wait()

            f = p if k > 0 else p - 1
            kf = (k - 1) % N_COLS
            f_exp = jnp.where(f == 3, 1, 0)
            f_side = jnp.where(f >= 2, 1, 0)
            base_slot = jnp.where(f >= 1, 1, tok_n)
            src0 = jnp.where(f < 1, 0, jnp.where(f == 1, 2, RECV + 3 * f_exp + 1))
            src1 = jnp.where(f < 1, 0, RECV + 3 * f_exp + 2 * f_side)

            @pl.when(f >= 1)
            def _():
                y_copy(f_exp, 2 * f_side + 1, 0, kf, me).wait_recv()

            @pl.when(f >= 2)
            def _():
                y_copy(f_exp, 2, 0, kf, me).wait_recv()

            if k > 0:
                @pl.when(h + 4 < 2 * N_PHASE * N_COLS)
                def _():
                    dn_start(h + 4)

            if k > 1:
                @pl.when(p == 1)
                def _():
                    gu_start(1, (5, 6) if k == 2 else (7,))

            if k != 1:
                @pl.when(p == 0)
                def _():
                    relay(max(k, 1))

            acc[:, kf * cw : (kf + 1) * cw] = folded(jnp.maximum(f, 0), base_slot, (src0, src1), kf)
            for i in range(2):
                y = jnp.dot(hid[...], dn[(h + i) % DN_SLOTS], preferred_element_type=F32).astype(BF)
                for half in range(2):
                    buf[work + half, :, k * cw + i * hw : k * cw + (i + 1) * hw] = y[half * cap : (half + 1) * cap]
            y_copy(exp, 2 * side + 1, work + 1, k, base_partner).start()

            @pl.when(side == 1)
            def _():
                y_copy(exp, 2, work, k, base).start()
        return carry

    lax.fori_loop(0, N_PHASE, phase_step, 0)

    for k in range(N_COLS):
        y_copy(0, 1, 3, k, partner).wait_send()
    outs = []
    for k in range(N_COLS):
        y_copy(1, 1, 1, k, partner).wait_recv()
        cols = slice(k * cw, (k + 1) * cw)
        total = None
        if k == N_COLS - 1:
            for peer in (2, 3):
                y_copy(1, peer, 0, k, me).wait_recv()
            total = folded(3, 1, (RECV + 4, RECV + 5), k)
        total = folded(0, 1, (0, RECV + 3), k, total).astype(BF)
        for half in range(2):
            buf[2 + half, :, cols] = total[half * cap : (half + 1) * cap]
        outs.append(pltpu.make_async_copy(buf.at[pl.ds(2, 2), :, cols], out_hbm.at[:, :, cols], s_out.at[k]))
        outs[k].start()

    for c in x_copies + m_copies + [p_copy]:
        c.wait_send()
    for exp in range(2):
        for peer in range(1, 4):
            for k in range(N_COLS):
                if exp + peer > 1:
                    y_copy(exp, peer, 0, k, devs[peer]).wait_send()
    for c in outs:
        c.wait()


def solution(mesh):
    row_spec = P(("dp", "ep"))

    def local_step(tokens, expert_ids, gate_w, route_counts, w_gate, w_up, w_down):
        tok_n, dim = tokens.shape
        ffn = w_gate.shape[2]
        cap = tok_n // 2
        cw = dim // N_COLS
        vmem = pl.BlockSpec(memory_space=pltpu.VMEM)
        hbm = pl.BlockSpec(memory_space=pl.ANY)
        dma = pltpu.SemaphoreType.DMA
        return pl.pallas_call(
            kernel,
            name="moe",
            out_shape=jax.ShapeDtypeStruct((2, cap, dim), BF),
            in_specs=[hbm, vmem, vmem, vmem, hbm, hbm, hbm],
            out_specs=hbm,
            scratch_shapes=[
                pltpu.VMEM((RECV + 6, cap, dim), BF),
                pltpu.VMEM((4, 8, tok_n), F32),
                pltpu.VMEM((4, tok_n, 4), F32),
                pltpu.VMEM((2 * cap, ffn), BF),
                pltpu.VMEM((tok_n, dim), F32),
                pltpu.VMEM((GU_SLOTS, 2, dim, F_BLOCK), BF),
                pltpu.VMEM((DN_SLOTS, ffn, cw // 2), BF),
                dma, dma((GU_SLOTS, 2)), dma((DN_SLOTS,)),
                dma((N_CHUNKS,)), dma((N_CHUNKS,)), dma, dma,
                dma((N_CHUNKS,)), dma((N_CHUNKS,)), dma((3,)), dma((3,)),
                dma((2, 4, N_COLS)), dma((2, 4, N_COLS)), dma((N_COLS,)),
            ],
            compiler_params=pltpu.CompilerParams(
                collective_id=0, has_side_effects=True, vmem_limit_bytes=67_000_000
            ),
        )(tokens.reshape(2, cap, dim), expert_ids.T, gate_w.T, route_counts, w_gate, w_up, w_down).reshape(tok_n, dim)

    return jax.shard_map(local_step, mesh=mesh, in_specs=(row_spec, row_spec, row_spec, row_spec, P("ep"), P("ep"), P("ep")), out_specs=row_spec, check_vma=False)
```

```python
import jax
import jax.numpy as jnp
from jax import lax
from jax.experimental import pallas as pl
from jax.experimental.pallas import tpu as pltpu
from jax.sharding import PartitionSpec as P

N_CHUNKS = 4
N_COLS = 4
GU_SLOTS = 8
DN_SLOTS = 6
F_BLOCK = 512
GROUPS = ((0, 2), (2, 5), (5, 8), (8, 11))
BF = jnp.bfloat16
F32 = jnp.float32
N_PHASE = 4
FOLDS = ((1, 0), (0, 0), (0, 1), (1, 1))
RECV = 8


def kernel(
    tok_hbm, ids_ref, gate_ref, cnt_ref, wg_hbm, wu_hbm, wd_hbm, acc,
    buf, maps, gates, hid, gu, dn,
    s_own, s_gu, s_dn, xs_send, xs_recv, ps_send, ps_recv, rs_send, rs_recv, ms_send, ms_recv, ys_send, ys_recv,
):
    _, cap, dim = tok_hbm.shape
    tok_n = 2 * cap
    ffn = wg_hbm.shape[2]
    n_gu = ffn // F_BLOCK
    chunk = tok_n // N_CHUNKS
    cw = dim // N_COLS
    hw = cw // 2

    me = lax.axis_index("ep")
    partner = me + 1 - 2 * (me % 2)
    across = (me + 2) % 4
    diagonal = (partner + 2) % 4
    devs = (me, partner, across, diagonal)

    def remote(src, dst, send, recv, dev):
        return pltpu.make_async_remote_copy(
            src_ref=src, dst_ref=dst, send_sem=send, recv_sem=recv,
            device_id={"ep": dev}, device_id_type=pl.DeviceIdType.MESH,
        )

    def gu_slot(exp, blk):
        return jnp.where(exp == 0, blk % GU_SLOTS, (GU_SLOTS - 1 + n_gu * GU_SLOTS - blk) % GU_SLOTS)

    def gu_copies(exp, blk):
        cols = pl.ds(pl.multiple_of(blk * F_BLOCK, F_BLOCK), F_BLOCK)
        slot = gu_slot(exp, blk)
        return (
            pltpu.make_async_copy(wg_hbm.at[exp, :, cols], gu.at[slot, 0], s_gu.at[slot, 0]),
            pltpu.make_async_copy(wu_hbm.at[exp, :, cols], gu.at[slot, 1], s_gu.at[slot, 1]),
        )

    def gu_start(exp, blks):
        for blk in blks:
            for c in gu_copies(exp, blk):
                c.start()

    def dn_copy(h):
        cols = pl.ds(pl.multiple_of((h % (2 * N_COLS)) * hw, hw), hw)
        slot = h % DN_SLOTS
        return pltpu.make_async_copy(wd_hbm.at[h // (4 * N_COLS), :, cols], dn.at[slot], s_dn.at[slot])

    def dn_start(h):
        dn_copy(h).start()
        dn_copy(h + 1).start()

    own_copy = pltpu.make_async_copy(tok_hbm, buf.at[pl.ds(0, 2)], s_own)
    own_copy.start()
    gu_start(0, range(2))

    barrier = pltpu.get_barrier_semaphore()
    for peer in (1, 2, 3):
        pl.semaphore_signal(barrier, inc=1, device_id={"ep": devs[peer]}, device_id_type=pl.DeviceIdType.MESH)
    pl.semaphore_wait(barrier, 3)

    def rows_of(peer, c):
        return buf.at[2 * peer + c // (N_CHUNKS // 2), pl.ds(c % (N_CHUNKS // 2) * chunk, chunk)]

    x_copies = [
        remote(tok_hbm.at[c // (N_CHUNKS // 2), pl.ds(c % (N_CHUNKS // 2) * chunk, chunk)], rows_of(2, c), xs_send.at[c], xs_recv.at[c], across)
        for c in range(N_CHUNKS)
    ]
    r_copies = [remote(rows_of(2, c), rows_of(3, c), rs_send.at[c], rs_recv.at[c], partner) for c in range(N_CHUNKS)]
    p_copy = remote(tok_hbm, buf.at[pl.ds(2, 2)], ps_send, ps_recv, partner)
    x_copies[0].start()
    p_copy.start()
    for c in range(1, N_CHUNKS):
        x_copies[c].start()

    row = lax.broadcasted_iota(jnp.int32, (8, 1), 0)
    exp_row = row % 2 + 2 * jnp.where(row < 2, devs[0], jnp.where(row < 4, devs[1], jnp.where(row < 6, devs[2], devs[3])))
    hit0 = ids_ref[0:1, :] == exp_row
    hit1 = ids_ref[1:2, :] == exp_row
    hit = jnp.where(hit0 | hit1, 1.0, 0.0)
    earlier = jnp.where(
        lax.broadcasted_iota(jnp.int32, (tok_n, tok_n), 0) < lax.broadcasted_iota(jnp.int32, (tok_n, tok_n), 1), 1.0, 0.0
    ).astype(BF)
    slot = jnp.dot(hit.astype(BF), earlier, preferred_element_type=F32)
    limit = jnp.sum(jnp.where(exp_row == lax.broadcasted_iota(jnp.int32, (8, 8), 1), cnt_ref[...], 0), axis=1, keepdims=True)
    served = (hit > 0.0) & (slot < limit.astype(F32))
    slot1 = jnp.where(served, slot + 1.0, 0.0)
    maps[0] = slot1
    m_copies = [remote(maps.at[0], maps.at[r], ms_send.at[r - 1], ms_recv.at[r - 1], devs[r]) for r in (1, 2, 3)]
    for c in m_copies:
        c.start()
    gates_t = (jnp.where(hit0, gate_ref[0:1, :], 0.0) + jnp.where(hit1, gate_ref[1:2, :], 0.0)).T
    slot1_t = slot1.T
    for f, (exp, side) in enumerate(FOLDS):
        for half in range(2):
            i = 2 * (2 * side + half) + exp
            gates[f, :, half : half + 1] = gates_t[:, i : i + 1]
            gates[f, :, 2 + half : 3 + half] = slot1_t[:, i : i + 1]
    own_copy.wait()
    gu_start(0, range(2, 5))
    for k in range(N_COLS):
        for half in range(2):
            acc[half * cap : (half + 1) * cap, k * cw : (k + 1) * cw] = buf[half, :, k * cw : (k + 1) * cw].astype(F32)

    def relay(c):
        x_copies[c].wait_recv()
        r_copies[c].start()

    def y_copy(exp, peer, part, k, dev):
        cols = pl.ds(k * cw, cw)
        return remote(buf.at[part, :, cols], buf.at[RECV + 3 * exp + peer - 1, :, cols], ys_send.at[exp, peer, k], ys_recv.at[exp, peer, k], dev)

    def fold(f, base_slot, srcs, k):
        lane = (lax.broadcasted_iota(jnp.int32, (tok_n, cap), 1) + base_slot).astype(F32)
        combs = [jnp.where(gates[f, :, 2 + half : 3 + half] == lane, 1.0, 0.0).astype(BF) for half in range(2)]
        for i in range(2):
            cols = slice(k * cw + i * hw, k * cw + (i + 1) * hw)
            total = acc[:, cols]
            for half in range(2):
                picked = jnp.dot(combs[half], buf[srcs[half], :, cols], preferred_element_type=F32)
                total += gates[f, :, half : half + 1] * picked
            acc[:, cols] = total

    def gather(side):
        slots = lax.broadcasted_iota(jnp.int32, (cap, tok_n), 0).astype(F32) + 1.0
        picks = [
            [
                jnp.where(maps[2 * side + half, pl.ds(2 * (2 * side + half) + exp, 1), :] == slots, 1.0, 0.0).astype(BF)
                for half in range(2)
            ]
            for exp in range(2)
        ]
        for k in range(2 * N_COLS):
            cols = slice(k * hw, (k + 1) * hw)
            toks = [buf[pl.ds(4 * side + 2 * half, 2), :, cols].reshape(tok_n, hw) for half in range(2)]
            got = [[jnp.dot(picks[exp][half], toks[half], preferred_element_type=F32).astype(BF) for half in range(2)] for exp in range(2)]
            for exp in range(2):
                for half in range(2):
                    buf[4 * side + 2 * (1 - exp) + half, :, cols] = got[exp][half]

    def phase_step(p, carry):
        exp = p // 2
        rev = p % 2
        side = ((p + 1) // 2) % 2
        base = jnp.where(side == 0, me, across)
        base_partner = jnp.where(side == 0, partner, diagonal)

        work = 4 * side + 2 * (1 - exp)

        @pl.when(p == 0)
        def _():
            p_copy.wait_recv()
            m_copies[0].wait_recv()

        @pl.when(p == 1)
        def _():
            m_copies[1].wait_recv()
            m_copies[2].wait_recv()
            for c in r_copies:
                c.wait_recv()
                c.wait_send()

        @pl.when(p < 2)
        def _():
            gather(side)

        def blk_of(s):
            return s + rev * (n_gu - 1 - 2 * s)

        for n, (first, last) in enumerate(GROUPS):
            @pl.when((rev == 0) | (n == 3))
            def _():
                for s in range(first, last):
                    for c in gu_copies(exp, blk_of(s)):
                        c.wait()

            @pl.when(p == 0)
            def _():
                if n == 0:
                    gu_start(0, (5, 6, 7))
                elif n == 1:
                    gu_start(0, (8, 9))
                elif n == 2:
                    gu_start(0, (10,))
                    dn_start(0)
                else:
                    dn_start(2)
                    relay(0)

            @pl.when(p == 1)
            def _():
                if n == 1:
                    gu_start(0, (2, 1))
                elif n == 2:
                    gu_start(0, (0,))
                    gu_start(1, (0, 1))
                elif n == 3:
                    gu_start(1, (2, 3, 4))

            @pl.when(p == 2)
            def _():
                if n == 1:
                    gu_start(1, (8, 9))
                elif n == 2:
                    gu_start(1, (10,))

            @pl.when(p == 3)
            def _():
                if n == 1:
                    gu_start(1, (2, 1))
                elif n == 2:
                    gu_start(1, (0,))

            if n == 3:
                dn_start(p * 2 * N_COLS + 4)

            rows = buf.at[pl.ds(work, 2)]
            for s in range(first, last):
                sl = gu_slot(exp, blk_of(s))
                for i in range(2):
                    cols = slice(i * hw, (i + 1) * hw)
                    a = jnp.dot(rows[...].reshape(tok_n, dim), gu[sl, 0, :, cols], preferred_element_type=F32)
                    b = jnp.dot(rows[...].reshape(tok_n, dim), gu[sl, 1, :, cols], preferred_element_type=F32)
                    off = pl.multiple_of(blk_of(s) * F_BLOCK, F_BLOCK) + i * hw
                    hid[:, pl.ds(pl.multiple_of(off, hw), hw)] = (a * jax.nn.sigmoid(a) * b).astype(BF)

        for k in range(N_COLS):
            h = 2 * (p * N_COLS + k)
            for i in range(2):
                dn_copy(h + i).wait()

            f = p if k > 0 else p - 1
            kf = (k - 1) % N_COLS
            f_exp = jnp.where(f == 3, 1, 0)
            f_side = jnp.where(f >= 2, 1, 0)
            base_slot = jnp.where(f >= 1, 1, tok_n)
            src0 = jnp.where(f < 1, 0, jnp.where(f == 1, 2, RECV + 3 * f_exp + 1))
            src1 = jnp.where(f < 1, 0, RECV + 3 * f_exp + 2 * f_side)

            @pl.when(f >= 1)
            def _():
                y_copy(f_exp, 2 * f_side + 1, 0, kf, me).wait_recv()

            @pl.when(f >= 2)
            def _():
                y_copy(f_exp, 2, 0, kf, me).wait_recv()

            if k > 0:
                @pl.when(h + 4 < 2 * N_PHASE * N_COLS)
                def _():
                    dn_start(h + 4)

            if k > 1:
                @pl.when(p == 1)
                def _():
                    gu_start(1, (5, 6) if k == 2 else (7,))

            if k != 1:
                @pl.when(p == 0)
                def _():
                    relay(max(k, 1))

            fold(jnp.maximum(f, 0), base_slot, (src0, src1), kf)
            for i in range(2):
                y = jnp.dot(hid[...], dn[(h + i) % DN_SLOTS], preferred_element_type=F32).astype(BF)
                for half in range(2):
                    buf[work + half, :, k * cw + i * hw : k * cw + (i + 1) * hw] = y[half * cap : (half + 1) * cap]
            y_copy(exp, 2 * side + 1, work + 1, k, base_partner).start()

            @pl.when(side == 1)
            def _():
                y_copy(exp, 2, work, k, base).start()
        return carry

    lax.fori_loop(0, N_PHASE, phase_step, 0)

    for k in range(N_COLS):
        y_copy(1, 1, 1, k, partner).wait_recv()
        if k == N_COLS - 1:
            for peer in (2, 3):
                y_copy(1, peer, 0, k, me).wait_recv()
            fold(3, 1, (RECV + 4, RECV + 5), k)
        fold(0, 1, (0, RECV + 3), k)

    for c in x_copies + m_copies + [p_copy]:
        c.wait_send()
    for exp in range(2):
        for peer in range(1, 4):
            for k in range(N_COLS):
                y_copy(exp, peer, 0, k, devs[peer]).wait_send()


def solution(mesh):
    row_spec = P(("dp", "ep"))

    def local_step(tokens, expert_ids, gate_w, route_counts, w_gate, w_up, w_down):
        tok_n, dim = tokens.shape
        ffn = w_gate.shape[2]
        cap = tok_n // 2
        cw = dim // N_COLS
        vmem = pl.BlockSpec(memory_space=pltpu.VMEM)
        hbm = pl.BlockSpec(memory_space=pl.ANY)
        dma = pltpu.SemaphoreType.DMA
        return pl.pallas_call(
            kernel,
            name="moe",
            out_shape=pltpu.VMEM((tok_n, dim), F32),
            in_specs=[hbm, vmem, vmem, vmem, hbm, hbm, hbm],
            out_specs=vmem,
            scratch_shapes=[
                pltpu.VMEM((RECV + 6, cap, dim), BF),
                pltpu.VMEM((4, 8, tok_n), F32),
                pltpu.VMEM((4, tok_n, 4), F32),
                pltpu.VMEM((2 * cap, ffn), BF),
                pltpu.VMEM((GU_SLOTS, 2, dim, F_BLOCK), BF),
                pltpu.VMEM((DN_SLOTS, ffn, cw // 2), BF),
                dma, dma((GU_SLOTS, 2)), dma((DN_SLOTS,)),
                dma((N_CHUNKS,)), dma((N_CHUNKS,)), dma, dma,
                dma((N_CHUNKS,)), dma((N_CHUNKS,)), dma((3,)), dma((3,)),
                dma((2, 4, N_COLS)), dma((2, 4, N_COLS)),
            ],
            compiler_params=pltpu.CompilerParams(
                collective_id=0, has_side_effects=True, vmem_limit_bytes=64_900_000
            ),
        )(tokens.reshape(2, cap, dim), expert_ids.T, gate_w.T, route_counts, w_gate, w_up, w_down).astype(BF)

    return jax.shard_map(local_step, mesh=mesh, in_specs=(row_spec, row_spec, row_spec, row_spec, P("ep"), P("ep"), P("ep")), out_specs=row_spec, check_vma=False)
```

```python
import jax
import jax.numpy as jnp
from jax import lax
from jax.experimental import pallas as pl
from jax.experimental.pallas import tpu as pltpu
from jax.sharding import PartitionSpec as P

N_CHUNKS = 8
N_COLS = 4
GU_SLOTS = 8
DN_SLOTS = 6
F_BLOCK = 512
GROUPS = ((0, 2), (2, 5), (5, 8), (8, 11))
BF = jnp.bfloat16
F32 = jnp.float32
N_PHASE = 4
FOLDS = ((1, 0), (0, 0), (0, 1), (1, 1))
RECV = 8


def kernel(
    tok_hbm, ids_ref, gate_ref, cnt_ref, wg_hbm, wu_hbm, wd_hbm, acc,
    buf, maps, gates, hid, gu, dn,
    s_own, s_gu, s_dn, xs_send, xs_recv, ps_send, ps_recv, rs_send, rs_recv, ms_send, ms_recv, ys_send, ys_recv,
):
    _, cap, dim = tok_hbm.shape
    tok_n = 2 * cap
    ffn = wg_hbm.shape[2]
    n_gu = ffn // F_BLOCK
    chunk = tok_n // N_CHUNKS
    cw = dim // N_COLS
    hw = cw // 2

    me = lax.axis_index("ep")
    partner = me + 1 - 2 * (me % 2)
    across = (me + 2) % 4
    diagonal = (partner + 2) % 4
    devs = (me, partner, across, diagonal)

    def remote(src, dst, send, recv, dev):
        return pltpu.make_async_remote_copy(
            src_ref=src, dst_ref=dst, send_sem=send, recv_sem=recv,
            device_id={"ep": dev}, device_id_type=pl.DeviceIdType.MESH,
        )

    def gu_slot(exp, blk):
        return jnp.where(exp == 0, blk % GU_SLOTS, (GU_SLOTS - 1 + n_gu * GU_SLOTS - blk) % GU_SLOTS)

    def gu_copies(exp, blk):
        cols = pl.ds(pl.multiple_of(blk * F_BLOCK, F_BLOCK), F_BLOCK)
        slot = gu_slot(exp, blk)
        return (
            pltpu.make_async_copy(wg_hbm.at[exp, :, cols], gu.at[slot, 0], s_gu.at[slot, 0]),
            pltpu.make_async_copy(wu_hbm.at[exp, :, cols], gu.at[slot, 1], s_gu.at[slot, 1]),
        )

    def gu_start(exp, blks):
        for blk in blks:
            for c in gu_copies(exp, blk):
                c.start()

    def dn_copy(h):
        cols = pl.ds(pl.multiple_of((h % (2 * N_COLS)) * hw, hw), hw)
        slot = h % DN_SLOTS
        return pltpu.make_async_copy(wd_hbm.at[h // (4 * N_COLS), :, cols], dn.at[slot], s_dn.at[slot])

    def dn_start(h):
        dn_copy(h).start()
        dn_copy(h + 1).start()

    own_copy = pltpu.make_async_copy(tok_hbm, buf.at[pl.ds(0, 2)], s_own)
    own_copy.start()
    gu_start(0, range(2))

    barrier = pltpu.get_barrier_semaphore()
    for peer in (1, 2, 3):
        pl.semaphore_signal(barrier, inc=1, device_id={"ep": devs[peer]}, device_id_type=pl.DeviceIdType.MESH)
    pl.semaphore_wait(barrier, 3)

    def rows_of(peer, c):
        return buf.at[2 * peer + c // (N_CHUNKS // 2), pl.ds(c % (N_CHUNKS // 2) * chunk, chunk)]

    x_copies = [
        remote(tok_hbm.at[c // (N_CHUNKS // 2), pl.ds(c % (N_CHUNKS // 2) * chunk, chunk)], rows_of(2, c), xs_send.at[c], xs_recv.at[c], across)
        for c in range(N_CHUNKS)
    ]
    r_copies = [remote(rows_of(2, c), rows_of(3, c), rs_send.at[c], rs_recv.at[c], partner) for c in range(N_CHUNKS)]
    p_copy = remote(tok_hbm, buf.at[pl.ds(2, 2)], ps_send, ps_recv, partner)
    x_copies[0].start()
    p_copy.start()
    for c in range(1, N_CHUNKS):
        x_copies[c].start()

    row = lax.broadcasted_iota(jnp.int32, (8, 1), 0)
    exp_row = row % 2 + 2 * jnp.where(row < 2, devs[0], jnp.where(row < 4, devs[1], jnp.where(row < 6, devs[2], devs[3])))
    hit0 = ids_ref[0:1, :] == exp_row
    hit1 = ids_ref[1:2, :] == exp_row
    hit = jnp.where(hit0 | hit1, 1.0, 0.0)
    earlier = jnp.where(
        lax.broadcasted_iota(jnp.int32, (tok_n, tok_n), 0) < lax.broadcasted_iota(jnp.int32, (tok_n, tok_n), 1), 1.0, 0.0
    ).astype(BF)
    slot = jnp.dot(hit.astype(BF), earlier, preferred_element_type=F32)
    limit = jnp.sum(jnp.where(exp_row == lax.broadcasted_iota(jnp.int32, (8, 8), 1), cnt_ref[...], 0), axis=1, keepdims=True)
    served = (hit > 0.0) & (slot < limit.astype(F32))
    slot1 = jnp.where(served, slot + 1.0, 0.0)
    maps[0] = slot1
    m_copies = [remote(maps.at[0], maps.at[r], ms_send.at[r - 1], ms_recv.at[r - 1], devs[r]) for r in (1, 2, 3)]
    for c in m_copies:
        c.start()
    gates_t = (jnp.where(hit0, gate_ref[0:1, :], 0.0) + jnp.where(hit1, gate_ref[1:2, :], 0.0)).T
    slot1_t = slot1.T
    for f, (exp, side) in enumerate(FOLDS):
        for half in range(2):
            i = 2 * (2 * side + half) + exp
            gates[f, :, half : half + 1] = gates_t[:, i : i + 1]
            gates[f, :, 2 + half : 3 + half] = slot1_t[:, i : i + 1]
    own_copy.wait()
    gu_start(0, range(2, 5))
    for k in range(N_COLS):
        for half in range(2):
            acc[half * cap : (half + 1) * cap, k * cw : (k + 1) * cw] = buf[half, :, k * cw : (k + 1) * cw].astype(F32)

    def relay(c):
        x_copies[c].wait_recv()
        r_copies[c].start()

    def y_copy(exp, peer, part, k, dev):
        cols = pl.ds(k * cw, cw)
        return remote(buf.at[part, :, cols], buf.at[RECV + 3 * exp + peer - 1, :, cols], ys_send.at[exp, peer, k], ys_recv.at[exp, peer, k], dev)

    def fold(f, base_slot, srcs, k):
        lane = (lax.broadcasted_iota(jnp.int32, (tok_n, cap), 1) + base_slot).astype(F32)
        combs = [jnp.where(gates[f, :, 2 + half : 3 + half] == lane, 1.0, 0.0).astype(BF) for half in range(2)]
        for i in range(2):
            cols = slice(k * cw + i * hw, k * cw + (i + 1) * hw)
            total = acc[:, cols]
            for half in range(2):
                picked = jnp.dot(combs[half], buf[srcs[half], :, cols], preferred_element_type=F32)
                total += gates[f, :, half : half + 1] * picked
            acc[:, cols] = total

    def gather(side):
        slots = lax.broadcasted_iota(jnp.int32, (cap, tok_n), 0).astype(F32) + 1.0
        picks = [
            [
                jnp.where(maps[2 * side + half, pl.ds(2 * (2 * side + half) + exp, 1), :] == slots, 1.0, 0.0).astype(BF)
                for half in range(2)
            ]
            for exp in range(2)
        ]
        for k in range(2 * N_COLS):
            cols = slice(k * hw, (k + 1) * hw)
            toks = [buf[pl.ds(4 * side + 2 * half, 2), :, cols].reshape(tok_n, hw) for half in range(2)]
            got = [[jnp.dot(picks[exp][half], toks[half], preferred_element_type=F32).astype(BF) for half in range(2)] for exp in range(2)]
            for exp in range(2):
                for half in range(2):
                    buf[4 * side + 2 * (1 - exp) + half, :, cols] = got[exp][half]

    def phase_step(p, carry):
        exp = p // 2
        rev = p % 2
        side = ((p + 1) // 2) % 2
        base = jnp.where(side == 0, me, across)
        base_partner = jnp.where(side == 0, partner, diagonal)

        work = 4 * side + 2 * (1 - exp)

        @pl.when(p == 0)
        def _():
            p_copy.wait_recv()
            m_copies[0].wait_recv()

        @pl.when(p == 1)
        def _():
            m_copies[1].wait_recv()
            m_copies[2].wait_recv()
            for c in r_copies:
                c.wait_recv()
                c.wait_send()

        @pl.when(p < 2)
        def _():
            gather(side)

        def blk_of(s):
            return s + rev * (n_gu - 1 - 2 * s)

        for n, (first, last) in enumerate(GROUPS):
            @pl.when((rev == 0) | (n == 3))
            def _():
                for s in range(first, last):
                    for c in gu_copies(exp, blk_of(s)):
                        c.wait()

            @pl.when(p == 0)
            def _():
                if n == 0:
                    gu_start(0, (5, 6, 7))
                elif n == 1:
                    gu_start(0, (8, 9))
                elif n == 2:
                    gu_start(0, (10,))
                    dn_start(0)
                else:
                    dn_start(2)
                    for c in range(3):
                        relay(c)

            @pl.when(p == 1)
            def _():
                if n == 1:
                    gu_start(0, (2, 1))
                elif n == 2:
                    gu_start(0, (0,))
                    gu_start(1, (0, 1))
                elif n == 3:
                    gu_start(1, (2, 3, 4))

            @pl.when(p == 2)
            def _():
                if n == 1:
                    gu_start(1, (8, 9))
                elif n == 2:
                    gu_start(1, (10,))

            @pl.when(p == 3)
            def _():
                if n == 1:
                    gu_start(1, (2, 1))
                elif n == 2:
                    gu_start(1, (0,))

            if n == 3:
                dn_start(p * 2 * N_COLS + 4)

            rows = buf.at[pl.ds(work, 2)]
            for s in range(first, last):
                sl = gu_slot(exp, blk_of(s))
                for i in range(2):
                    cols = slice(i * hw, (i + 1) * hw)
                    a = jnp.dot(rows[...].reshape(tok_n, dim), gu[sl, 0, :, cols], preferred_element_type=F32)
                    b = jnp.dot(rows[...].reshape(tok_n, dim), gu[sl, 1, :, cols], preferred_element_type=F32)
                    off = pl.multiple_of(blk_of(s) * F_BLOCK, F_BLOCK) + i * hw
                    hid[:, pl.ds(pl.multiple_of(off, hw), hw)] = (a * jax.nn.sigmoid(a) * b).astype(BF)

        for k in range(N_COLS):
            h = 2 * (p * N_COLS + k)
            for i in range(2):
                dn_copy(h + i).wait()

            f = p if k > 0 else p - 1
            kf = (k - 1) % N_COLS
            f_exp = jnp.where(f == 3, 1, 0)
            f_side = jnp.where(f >= 2, 1, 0)
            base_slot = jnp.where(f >= 1, 1, tok_n)
            src0 = jnp.where(f < 1, 0, jnp.where(f == 1, 2, RECV + 3 * f_exp + 1))
            src1 = jnp.where(f < 1, 0, RECV + 3 * f_exp + 2 * f_side)

            @pl.when(f >= 1)
            def _():
                y_copy(f_exp, 2 * f_side + 1, 0, kf, me).wait_recv()

            @pl.when(f >= 2)
            def _():
                y_copy(f_exp, 2, 0, kf, me).wait_recv()

            if k > 0:
                @pl.when(h + 4 < 2 * N_PHASE * N_COLS)
                def _():
                    dn_start(h + 4)

            if k > 1:
                @pl.when(p == 1)
                def _():
                    gu_start(1, (5, 6) if k == 2 else (7,))

            @pl.when(p == 0)
            def _():
                for c in ((3,), (4,), (5, 6), (7,))[k]:
                    relay(c)

            fold(jnp.maximum(f, 0), base_slot, (src0, src1), kf)
            for i in range(2):
                y = jnp.dot(hid[...], dn[(h + i) % DN_SLOTS], preferred_element_type=F32).astype(BF)
                for half in range(2):
                    buf[work + half, :, k * cw + i * hw : k * cw + (i + 1) * hw] = y[half * cap : (half + 1) * cap]
            y_copy(exp, 2 * side + 1, work + 1, k, base_partner).start()

            @pl.when(side == 1)
            def _():
                y_copy(exp, 2, work, k, base).start()
        return carry

    lax.fori_loop(0, N_PHASE, phase_step, 0)

    for c in x_copies + m_copies + [p_copy]:
        c.wait_send()

    def sent(exp, peer):
        for k in range(N_COLS):
            y_copy(exp, peer, 0, k, devs[peer]).wait_send()

    for peer in range(1, 4):
        sent(0, peer)
    for k in range(N_COLS):
        y_copy(1, 1, 1, k, partner).wait_recv()
        fold(0, 1, (0, RECV + 3), k)
    sent(1, 1)
    for peer in (2, 3):
        y_copy(1, peer, 0, N_COLS - 1, me).wait_recv()
    fold(3, 1, (RECV + 4, RECV + 5), N_COLS - 1)
    for peer in (2, 3):
        sent(1, peer)


def solution(mesh):
    row_spec = P(("dp", "ep"))

    def local_step(tokens, expert_ids, gate_w, route_counts, w_gate, w_up, w_down):
        tok_n, dim = tokens.shape
        ffn = w_gate.shape[2]
        cap = tok_n // 2
        cw = dim // N_COLS
        vmem = pl.BlockSpec(memory_space=pltpu.VMEM)
        hbm = pl.BlockSpec(memory_space=pl.ANY)
        dma = pltpu.SemaphoreType.DMA
        return pl.pallas_call(
            kernel,
            name="moe",
            out_shape=pltpu.VMEM((tok_n, dim), F32),
            in_specs=[hbm, vmem, vmem, vmem, hbm, hbm, hbm],
            out_specs=vmem,
            scratch_shapes=[
                pltpu.VMEM((RECV + 6, cap, dim), BF),
                pltpu.VMEM((4, 8, tok_n), F32),
                pltpu.VMEM((4, tok_n, 4), F32),
                pltpu.VMEM((2 * cap, ffn), BF),
                pltpu.VMEM((GU_SLOTS, 2, dim, F_BLOCK), BF),
                pltpu.VMEM((DN_SLOTS, ffn, cw // 2), BF),
                dma, dma((GU_SLOTS, 2)), dma((DN_SLOTS,)),
                dma((N_CHUNKS,)), dma((N_CHUNKS,)), dma, dma,
                dma((N_CHUNKS,)), dma((N_CHUNKS,)), dma((3,)), dma((3,)),
                dma((2, 4, N_COLS)), dma((2, 4, N_COLS)),
            ],
            compiler_params=pltpu.CompilerParams(
                collective_id=0, has_side_effects=True, vmem_limit_bytes=64_900_000
            ),
        )(tokens.reshape(2, cap, dim), expert_ids.T, gate_w.T, route_counts, w_gate, w_up, w_down).astype(BF)

    return jax.shard_map(local_step, mesh=mesh, in_specs=(row_spec, row_spec, row_spec, row_spec, P("ep"), P("ep"), P("ep")), out_specs=row_spec, check_vma=False)
```

```python
import jax
import jax.numpy as jnp
from jax import lax
from jax.experimental import pallas as pl
from jax.experimental.pallas import tpu as pltpu
from jax.sharding import PartitionSpec as P

N_CHUNKS = 4
N_COLS = 4
GU_SLOTS = 8
DN_SLOTS = 6
F_BLOCK = 512
GROUPS = ((0, 2), (2, 5), (5, 8), (8, 11))
BF = jnp.bfloat16
F32 = jnp.float32
N_PHASE = 4
FOLDS = ((1, 0), (0, 0), (0, 1), (1, 1))
RECV = 8


def kernel(
    tok_hbm, ids_ref, gate_ref, cnt_ref, wg_hbm, wu_hbm, wd_hbm, acc,
    buf, maps, comb, gates, hid, gu, dn,
    s_own, s_gu, s_dn, xs_send, xs_recv, ps_send, ps_recv, rs_send, rs_recv, ms_send, ms_recv, ys_send, ys_recv,
):
    _, cap, dim = tok_hbm.shape
    tok_n = 2 * cap
    ffn = wg_hbm.shape[2]
    n_gu = ffn // F_BLOCK
    chunk = tok_n // N_CHUNKS
    cw = dim // N_COLS
    hw = cw // 2

    me = lax.axis_index("ep")
    partner = me + 1 - 2 * (me % 2)
    across = (me + 2) % 4
    diagonal = (partner + 2) % 4
    devs = (me, partner, across, diagonal)

    def remote(src, dst, send, recv, dev):
        return pltpu.make_async_remote_copy(
            src_ref=src, dst_ref=dst, send_sem=send, recv_sem=recv,
            device_id={"ep": dev}, device_id_type=pl.DeviceIdType.MESH,
        )

    def gu_slot(exp, blk):
        return jnp.where(exp == 0, blk % GU_SLOTS, (GU_SLOTS - 1 + n_gu * GU_SLOTS - blk) % GU_SLOTS)

    def gu_copies(exp, blk):
        cols = pl.ds(pl.multiple_of(blk * F_BLOCK, F_BLOCK), F_BLOCK)
        slot = gu_slot(exp, blk)
        return (
            pltpu.make_async_copy(wg_hbm.at[exp, :, cols], gu.at[slot, 0], s_gu.at[slot, 0]),
            pltpu.make_async_copy(wu_hbm.at[exp, :, cols], gu.at[slot, 1], s_gu.at[slot, 1]),
        )

    def gu_start(exp, blks):
        for blk in blks:
            for c in gu_copies(exp, blk):
                c.start()

    def dn_copy(h):
        cols = pl.ds(pl.multiple_of((h % (2 * N_COLS)) * hw, hw), hw)
        slot = h % DN_SLOTS
        return pltpu.make_async_copy(wd_hbm.at[h // (4 * N_COLS), :, cols], dn.at[slot], s_dn.at[slot])

    def dn_start(h):
        dn_copy(h).start()
        dn_copy(h + 1).start()

    own_copy = pltpu.make_async_copy(tok_hbm, buf.at[pl.ds(0, 2)], s_own)
    own_copy.start()
    gu_start(0, range(2))

    barrier = pltpu.get_barrier_semaphore()
    for peer in (1, 2, 3):
        pl.semaphore_signal(barrier, inc=1, device_id={"ep": devs[peer]}, device_id_type=pl.DeviceIdType.MESH)
    pl.semaphore_wait(barrier, 3)

    def rows_of(peer, c):
        return buf.at[2 * peer + c // (N_CHUNKS // 2), pl.ds(c % (N_CHUNKS // 2) * chunk, chunk)]

    x_copies = [
        remote(tok_hbm.at[c // (N_CHUNKS // 2), pl.ds(c % (N_CHUNKS // 2) * chunk, chunk)], rows_of(2, c), xs_send.at[c], xs_recv.at[c], across)
        for c in range(N_CHUNKS)
    ]
    r_copies = [remote(rows_of(2, c), rows_of(3, c), rs_send.at[c], rs_recv.at[c], partner) for c in range(N_CHUNKS)]
    p_copy = remote(tok_hbm, buf.at[pl.ds(2, 2)], ps_send, ps_recv, partner)
    x_copies[0].start()
    p_copy.start()
    for c in range(1, N_CHUNKS):
        x_copies[c].start()

    row = lax.broadcasted_iota(jnp.int32, (8, 1), 0)
    exp_row = row % 2 + 2 * jnp.where(row < 2, devs[0], jnp.where(row < 4, devs[1], jnp.where(row < 6, devs[2], devs[3])))
    hit0 = ids_ref[0:1, :] == exp_row
    hit1 = ids_ref[1:2, :] == exp_row
    hit = jnp.where(hit0 | hit1, 1.0, 0.0)
    earlier = jnp.where(
        lax.broadcasted_iota(jnp.int32, (tok_n, tok_n), 0) < lax.broadcasted_iota(jnp.int32, (tok_n, tok_n), 1), 1.0, 0.0
    ).astype(BF)
    slot = jnp.dot(hit.astype(BF), earlier, preferred_element_type=F32)
    limit = jnp.sum(jnp.where(exp_row == lax.broadcasted_iota(jnp.int32, (8, 8), 1), cnt_ref[...], 0), axis=1, keepdims=True)
    served = (hit > 0.0) & (slot < limit.astype(F32))
    slot1 = jnp.where(served, slot + 1.0, 0.0)
    maps[0] = slot1
    m_copies = [remote(maps.at[0], maps.at[r], ms_send.at[r - 1], ms_recv.at[r - 1], devs[r]) for r in (1, 2, 3)]
    for c in m_copies:
        c.start()
    gates_t = (jnp.where(hit0, gate_ref[0:1, :], 0.0) + jnp.where(hit1, gate_ref[1:2, :], 0.0)).T
    slot1_t = slot1.T
    lane = lax.broadcasted_iota(jnp.int32, (tok_n, cap), 1).astype(F32) + 1.0
    comb[N_PHASE] = jnp.zeros((2, tok_n, cap), BF)
    for f, (exp, side) in enumerate(FOLDS):
        for half in range(2):
            i = 2 * (2 * side + half) + exp
            gates[f, :, half : half + 1] = gates_t[:, i : i + 1]
            comb[f, half] = jnp.where(slot1_t[:, i : i + 1] == lane, 1.0, 0.0).astype(BF)
    own_copy.wait()
    gu_start(0, range(2, 5))
    for k in range(N_COLS):
        for half in range(2):
            acc[half * cap : (half + 1) * cap, k * cw : (k + 1) * cw] = buf[half, :, k * cw : (k + 1) * cw].astype(F32)

    def relay(c):
        x_copies[c].wait_recv()
        r_copies[c].start()

    def y_copy(exp, peer, part, k, dev):
        cols = pl.ds(k * cw, cw)
        return remote(buf.at[part, :, cols], buf.at[RECV + 3 * exp + peer - 1, :, cols], ys_send.at[exp, peer, k], ys_recv.at[exp, peer, k], dev)

    def fold(f, c, srcs, k):
        for i in range(2):
            cols = slice(k * cw + i * hw, k * cw + (i + 1) * hw)
            total = acc[:, cols]
            for half in range(2):
                picked = jnp.dot(comb[c, half], buf[srcs[half], :, cols], preferred_element_type=F32)
                total += gates[f, :, half : half + 1] * picked
            acc[:, cols] = total

    def gather(side):
        slots = lax.broadcasted_iota(jnp.int32, (cap, tok_n), 0).astype(F32) + 1.0
        picks = [
            [
                jnp.where(maps[2 * side + half, pl.ds(2 * (2 * side + half) + exp, 1), :] == slots, 1.0, 0.0).astype(BF)
                for half in range(2)
            ]
            for exp in range(2)
        ]
        for k in range(2 * N_COLS):
            cols = slice(k * hw, (k + 1) * hw)
            toks = [buf[pl.ds(4 * side + 2 * half, 2), :, cols].reshape(tok_n, hw) for half in range(2)]
            got = [[jnp.dot(picks[exp][half], toks[half], preferred_element_type=F32).astype(BF) for half in range(2)] for exp in range(2)]
            for exp in range(2):
                for half in range(2):
                    buf[4 * side + 2 * (1 - exp) + half, :, cols] = got[exp][half]

    def phase_step(p, carry):
        exp = p // 2
        rev = p % 2
        side = ((p + 1) // 2) % 2
        base = jnp.where(side == 0, me, across)
        base_partner = jnp.where(side == 0, partner, diagonal)

        work = 4 * side + 2 * (1 - exp)

        @pl.when(p == 0)
        def _():
            p_copy.wait_recv()
            m_copies[0].wait_recv()

        @pl.when(p == 1)
        def _():
            m_copies[1].wait_recv()
            m_copies[2].wait_recv()
            for c in r_copies:
                c.wait_recv()
                c.wait_send()

        @pl.when(p < 2)
        def _():
            gather(side)

        def blk_of(s):
            return s + rev * (n_gu - 1 - 2 * s)

        for n, (first, last) in enumerate(GROUPS):
            @pl.when((rev == 0) | (n == 3))
            def _():
                for s in range(first, last):
                    for c in gu_copies(exp, blk_of(s)):
                        c.wait()

            @pl.when(p == 0)
            def _():
                if n == 0:
                    gu_start(0, (5, 6, 7))
                elif n == 1:
                    gu_start(0, (8, 9))
                elif n == 2:
                    gu_start(0, (10,))
                    dn_start(0)
                else:
                    dn_start(2)
                    relay(0)

            @pl.when(p == 1)
            def _():
                if n == 1:
                    gu_start(0, (2, 1))
                elif n == 2:
                    gu_start(0, (0,))
                    gu_start(1, (0, 1))
                elif n == 3:
                    gu_start(1, (2, 3, 4))

            @pl.when(p == 2)
            def _():
                if n == 1:
                    gu_start(1, (8, 9))
                elif n == 2:
                    gu_start(1, (10,))

            @pl.when(p == 3)
            def _():
                if n == 1:
                    gu_start(1, (2, 1))
                elif n == 2:
                    gu_start(1, (0,))

            if n == 3:
                dn_start(p * 2 * N_COLS + 4)

            rows = buf.at[pl.ds(work, 2)]
            for s in range(first, last):
                sl = gu_slot(exp, blk_of(s))
                for i in range(2):
                    cols = slice(i * hw, (i + 1) * hw)
                    a = jnp.dot(rows[...].reshape(tok_n, dim), gu[sl, 0, :, cols], preferred_element_type=F32)
                    b = jnp.dot(rows[...].reshape(tok_n, dim), gu[sl, 1, :, cols], preferred_element_type=F32)
                    off = pl.multiple_of(blk_of(s) * F_BLOCK, F_BLOCK) + i * hw
                    hid[:, pl.ds(pl.multiple_of(off, hw), hw)] = (a * jax.nn.sigmoid(a) * b).astype(BF)

        for k in range(N_COLS):
            h = 2 * (p * N_COLS + k)
            for i in range(2):
                dn_copy(h + i).wait()

            f = p if k > 0 else p - 1
            kf = (k - 1) % N_COLS
            f_exp = jnp.where(f == 3, 1, 0)
            f_side = jnp.where(f >= 2, 1, 0)
            f_comb = jnp.where(f >= 1, f, N_PHASE)
            src0 = jnp.where(f < 1, 0, jnp.where(f == 1, 2, RECV + 3 * f_exp + 1))
            src1 = jnp.where(f < 1, 0, RECV + 3 * f_exp + 2 * f_side)

            @pl.when(f >= 1)
            def _():
                y_copy(f_exp, 2 * f_side + 1, 0, kf, me).wait_recv()

            @pl.when(f >= 2)
            def _():
                y_copy(f_exp, 2, 0, kf, me).wait_recv()

            if k > 0:
                @pl.when(h + 4 < 2 * N_PHASE * N_COLS)
                def _():
                    dn_start(h + 4)

            if k > 1:
                @pl.when(p == 1)
                def _():
                    gu_start(1, (5, 6) if k == 2 else (7,))

            if k != 1:
                @pl.when(p == 0)
                def _():
                    relay(max(k, 1))

            fold(jnp.maximum(f, 0), f_comb, (src0, src1), kf)
            for i in range(2):
                y = jnp.dot(hid[...], dn[(h + i) % DN_SLOTS], preferred_element_type=F32).astype(BF)
                for half in range(2):
                    buf[work + half, :, k * cw + i * hw : k * cw + (i + 1) * hw] = y[half * cap : (half + 1) * cap]
            y_copy(exp, 2 * side + 1, work + 1, k, base_partner).start()

            @pl.when(side == 1)
            def _():
                y_copy(exp, 2, work, k, base).start()
        return carry

    lax.fori_loop(0, N_PHASE, phase_step, 0)

    for k in range(N_COLS):
        y_copy(1, 1, 1, k, partner).wait_recv()
        if k == N_COLS - 1:
            for peer in (2, 3):
                y_copy(1, peer, 0, k, me).wait_recv()
            fold(3, 3, (RECV + 4, RECV + 5), k)
        fold(0, 0, (0, RECV + 3), k)

    for c in x_copies + m_copies + [p_copy]:
        c.wait_send()
    for exp in range(2):
        for peer in range(1, 4):
            for k in range(N_COLS):
                y_copy(exp, peer, 0, k, devs[peer]).wait_send()


def solution(mesh):
    row_spec = P(("dp", "ep"))

    def local_step(tokens, expert_ids, gate_w, route_counts, w_gate, w_up, w_down):
        tok_n, dim = tokens.shape
        ffn = w_gate.shape[2]
        cap = tok_n // 2
        cw = dim // N_COLS
        vmem = pl.BlockSpec(memory_space=pltpu.VMEM)
        hbm = pl.BlockSpec(memory_space=pl.ANY)
        dma = pltpu.SemaphoreType.DMA
        return pl.pallas_call(
            kernel,
            name="moe",
            out_shape=pltpu.VMEM((tok_n, dim), F32),
            in_specs=[hbm, vmem, vmem, vmem, hbm, hbm, hbm],
            out_specs=vmem,
            scratch_shapes=[
                pltpu.VMEM((RECV + 6, cap, dim), BF),
                pltpu.VMEM((4, 8, tok_n), F32),
                pltpu.VMEM((N_PHASE + 1, 2, tok_n, cap), BF),
                pltpu.VMEM((4, tok_n, 2), F32),
                pltpu.VMEM((2 * cap, ffn), BF),
                pltpu.VMEM((GU_SLOTS, 2, dim, F_BLOCK), BF),
                pltpu.VMEM((DN_SLOTS, ffn, cw // 2), BF),
                dma, dma((GU_SLOTS, 2)), dma((DN_SLOTS,)),
                dma((N_CHUNKS,)), dma((N_CHUNKS,)), dma, dma,
                dma((N_CHUNKS,)), dma((N_CHUNKS,)), dma((3,)), dma((3,)),
                dma((2, 4, N_COLS)), dma((2, 4, N_COLS)),
            ],
            compiler_params=pltpu.CompilerParams(
                collective_id=0, has_side_effects=True, vmem_limit_bytes=64_900_000
            ),
        )(tokens.reshape(2, cap, dim), expert_ids.T, gate_w.T, route_counts, w_gate, w_up, w_down).astype(BF)

    return jax.shard_map(local_step, mesh=mesh, in_specs=(row_spec, row_spec, row_spec, row_spec, P("ep"), P("ep"), P("ep")), out_specs=row_spec, check_vma=False)
```

```python
import jax
import jax.numpy as jnp
from jax import lax
from jax.experimental import pallas as pl
from jax.experimental.pallas import tpu as pltpu
from jax.sharding import PartitionSpec as P

N_CHUNKS = 4
N_COLS = 4
GU_SLOTS = 8
DN_SLOTS = 6
F_BLOCK = 512
GROUPS = ((0, 2), (2, 5), (5, 8), (8, 11))
BF = jnp.bfloat16
F32 = jnp.float32
N_PHASE = 4
FOLDS = ((1, 0), (0, 0), (0, 1), (1, 1))
RECV = 8


def kernel(
    tok_hbm, ids_ref, gate_ref, cnt_ref, wg_hbm, wu_hbm, wd_hbm, acc,
    buf, maps, comb, gates, hid, gu, dn,
    s_own, s_gu, s_dn, xs_send, xs_recv, ps_send, ps_recv, rs_send, rs_recv, ms_send, ms_recv, ys_send, ys_recv,
):
    _, cap, dim = tok_hbm.shape
    tok_n = 2 * cap
    ffn = wg_hbm.shape[2]
    n_gu = ffn // F_BLOCK
    chunk = tok_n // N_CHUNKS
    cw = dim // N_COLS
    hw = cw // 2

    me = lax.axis_index("ep")
    partner = me + 1 - 2 * (me % 2)
    across = (me + 2) % 4
    diagonal = (partner + 2) % 4
    devs = (me, partner, across, diagonal)

    def remote(src, dst, send, recv, dev):
        return pltpu.make_async_remote_copy(
            src_ref=src, dst_ref=dst, send_sem=send, recv_sem=recv,
            device_id={"ep": dev}, device_id_type=pl.DeviceIdType.MESH,
        )

    def gu_slot(exp, blk):
        return jnp.where(exp == 0, blk % GU_SLOTS, (GU_SLOTS - 1 + n_gu * GU_SLOTS - blk) % GU_SLOTS)

    def gu_copies(exp, blk):
        cols = pl.ds(pl.multiple_of(blk * F_BLOCK, F_BLOCK), F_BLOCK)
        slot = gu_slot(exp, blk)
        return (
            pltpu.make_async_copy(wg_hbm.at[exp, :, cols], gu.at[slot, 0], s_gu.at[slot, 0]),
            pltpu.make_async_copy(wu_hbm.at[exp, :, cols], gu.at[slot, 1], s_gu.at[slot, 1]),
        )

    def gu_start(exp, blks):
        for blk in blks:
            for c in gu_copies(exp, blk):
                c.start()

    def dn_copy(h):
        cols = pl.ds(pl.multiple_of((h % (2 * N_COLS)) * hw, hw), hw)
        slot = h % DN_SLOTS
        return pltpu.make_async_copy(wd_hbm.at[h // (4 * N_COLS), :, cols], dn.at[slot], s_dn.at[slot])

    def dn_start(h):
        dn_copy(h).start()
        dn_copy(h + 1).start()

    own_copy = pltpu.make_async_copy(tok_hbm, buf.at[pl.ds(0, 2)], s_own)
    own_copy.start()
    gu_start(0, range(2))

    barrier = pltpu.get_barrier_semaphore()
    for peer in (1, 2, 3):
        pl.semaphore_signal(barrier, inc=1, device_id={"ep": devs[peer]}, device_id_type=pl.DeviceIdType.MESH)
    pl.semaphore_wait(barrier, 3)

    def rows_of(peer, c):
        return buf.at[2 * peer + c // (N_CHUNKS // 2), pl.ds(c % (N_CHUNKS // 2) * chunk, chunk)]

    x_copies = [
        remote(tok_hbm.at[c // (N_CHUNKS // 2), pl.ds(c % (N_CHUNKS // 2) * chunk, chunk)], rows_of(2, c), xs_send.at[c], xs_recv.at[c], across)
        for c in range(N_CHUNKS)
    ]
    r_copies = [remote(rows_of(2, c), rows_of(3, c), rs_send.at[c], rs_recv.at[c], partner) for c in range(N_CHUNKS)]
    p_copy = remote(tok_hbm, buf.at[pl.ds(2, 2)], ps_send, ps_recv, partner)
    x_copies[0].start()
    p_copy.start()
    for c in range(1, N_CHUNKS):
        x_copies[c].start()

    row = lax.broadcasted_iota(jnp.int32, (8, 1), 0)
    exp_row = row % 2 + 2 * jnp.where(row < 2, devs[0], jnp.where(row < 4, devs[1], jnp.where(row < 6, devs[2], devs[3])))
    hit0 = ids_ref[0:1, :] == exp_row
    hit1 = ids_ref[1:2, :] == exp_row
    hit = jnp.where(hit0 | hit1, 1.0, 0.0)
    earlier = jnp.where(
        lax.broadcasted_iota(jnp.int32, (tok_n, tok_n), 0) < lax.broadcasted_iota(jnp.int32, (tok_n, tok_n), 1), 1.0, 0.0
    ).astype(BF)
    slot = jnp.dot(hit.astype(BF), earlier, preferred_element_type=F32)
    limit = jnp.sum(jnp.where(exp_row == lax.broadcasted_iota(jnp.int32, (8, 8), 1), cnt_ref[...], 0), axis=1, keepdims=True)
    served = (hit > 0.0) & (slot < limit.astype(F32))
    slot1 = jnp.where(served, slot + 1.0, 0.0)
    maps[0] = slot1
    m_copies = [remote(maps.at[0], maps.at[r], ms_send.at[r - 1], ms_recv.at[r - 1], devs[r]) for r in (1, 2, 3)]
    for c in m_copies:
        c.start()
    gates_t = (jnp.where(hit0, gate_ref[0:1, :], 0.0) + jnp.where(hit1, gate_ref[1:2, :], 0.0)).T
    slot1_t = slot1.T
    lane = lax.broadcasted_iota(jnp.int32, (tok_n, cap), 1).astype(F32) + 1.0
    comb[N_PHASE] = jnp.zeros((2, tok_n, cap), BF)
    for f, (exp, side) in enumerate(FOLDS):
        for half in range(2):
            i = 2 * (2 * side + half) + exp
            gates[f, :, half : half + 1] = gates_t[:, i : i + 1]
            comb[f, half] = jnp.where(slot1_t[:, i : i + 1] == lane, 1.0, 0.0).astype(BF)
    own_copy.wait()
    gu_start(0, range(2, 5))
    for k in range(N_COLS):
        for half in range(2):
            acc[half * cap : (half + 1) * cap, k * cw : (k + 1) * cw] = buf[half, :, k * cw : (k + 1) * cw].astype(F32)

    def relay(c):
        x_copies[c].wait_recv()
        r_copies[c].start()

    def y_copy(exp, peer, part, k, dev):
        cols = pl.ds(k * cw, cw)
        return remote(buf.at[part, :, cols], buf.at[RECV + 3 * exp + peer - 1, :, cols], ys_send.at[exp, peer, k], ys_recv.at[exp, peer, k], dev)

    def fold(f, c, srcs, k):
        for i in range(2):
            cols = slice(k * cw + i * hw, k * cw + (i + 1) * hw)
            total = acc[:, cols]
            for half in range(2):
                picked = jnp.dot(comb[c, half], buf[srcs[half], :, cols], preferred_element_type=F32)
                total += gates[f, :, half : half + 1] * picked
            acc[:, cols] = total

    def gather(side):
        slots = lax.broadcasted_iota(jnp.int32, (cap, tok_n), 0).astype(F32) + 1.0
        picks = [
            [
                jnp.where(maps[2 * side + half, pl.ds(2 * (2 * side + half) + exp, 1), :] == slots, 1.0, 0.0).astype(BF)
                for half in range(2)
            ]
            for exp in range(2)
        ]
        for k in range(2 * N_COLS):
            cols = slice(k * hw, (k + 1) * hw)
            toks = [buf[pl.ds(4 * side + 2 * half, 2), :, cols].reshape(tok_n, hw) for half in range(2)]
            got = [[jnp.dot(picks[exp][half], toks[half], preferred_element_type=F32).astype(BF) for half in range(2)] for exp in range(2)]
            for exp in range(2):
                for half in range(2):
                    buf[4 * side + 2 * (1 - exp) + half, :, cols] = got[exp][half]

    def phase_step(p, carry):
        exp = p // 2
        rev = p % 2
        side = ((p + 1) // 2) % 2
        base = jnp.where(side == 0, me, across)
        base_partner = jnp.where(side == 0, partner, diagonal)

        work = 4 * side + 2 * (1 - exp)

        @pl.when(p == 0)
        def _():
            p_copy.wait_recv()
            m_copies[0].wait_recv()

        @pl.when(p == 1)
        def _():
            m_copies[1].wait_recv()
            m_copies[2].wait_recv()
            for c in r_copies:
                c.wait_recv()
                c.wait_send()

        @pl.when(p < 2)
        def _():
            gather(side)

        def blk_of(s):
            return s + rev * (n_gu - 1 - 2 * s)

        for n, (first, last) in enumerate(GROUPS):
            @pl.when((rev == 0) | (n == 3))
            def _():
                for s in range(first, last):
                    for c in gu_copies(exp, blk_of(s)):
                        c.wait()

            @pl.when(p == 0)
            def _():
                if n == 0:
                    gu_start(0, (5, 6, 7))
                elif n == 1:
                    gu_start(0, (8, 9))
                elif n == 2:
                    gu_start(0, (10,))
                    dn_start(0)
                else:
                    dn_start(2)
                    relay(0)

            @pl.when(p == 1)
            def _():
                if n == 1:
                    gu_start(0, (2, 1))
                elif n == 2:
                    gu_start(0, (0,))
                    gu_start(1, (0, 1))
                elif n == 3:
                    gu_start(1, (2, 3, 4))

            @pl.when(p == 2)
            def _():
                if n == 1:
                    gu_start(1, (8, 9))
                elif n == 2:
                    gu_start(1, (10,))

            @pl.when(p == 3)
            def _():
                if n == 1:
                    gu_start(1, (2, 1))
                elif n == 2:
                    gu_start(1, (0,))

            if n == 3:
                dn_start(p * 2 * N_COLS + 4)

            rows = buf.at[pl.ds(work, 2)]
            for s in range(first, last):
                sl = gu_slot(exp, blk_of(s))
                for i in range(2):
                    cols = slice(i * hw, (i + 1) * hw)
                    a = jnp.dot(rows[...].reshape(tok_n, dim), gu[sl, 0, :, cols], preferred_element_type=F32)
                    b = jnp.dot(rows[...].reshape(tok_n, dim), gu[sl, 1, :, cols], preferred_element_type=F32)
                    off = pl.multiple_of(blk_of(s) * F_BLOCK, F_BLOCK) + i * hw
                    hid[:, pl.ds(pl.multiple_of(off, hw), hw)] = (a * jax.nn.sigmoid(a) * b).astype(BF)

        for k in range(N_COLS):
            h = 2 * (p * N_COLS + k)
            for i in range(2):
                dn_copy(h + i).wait()

            f = p if k > 0 else p - 1
            kf = (k - 1) % N_COLS
            f_exp = jnp.where(f == 3, 1, 0)
            f_side = jnp.where(f >= 2, 1, 0)
            f_comb = jnp.where(f >= 1, f, N_PHASE)
            src0 = jnp.where(f < 1, 0, jnp.where(f == 1, 2, RECV + 3 * f_exp + 1))
            src1 = jnp.where(f < 1, 0, RECV + 3 * f_exp + 2 * f_side)

            @pl.when(f >= 1)
            def _():
                y_copy(f_exp, 2 * f_side + 1, 0, kf, me).wait_recv()

            @pl.when(f >= 2)
            def _():
                y_copy(f_exp, 2, 0, kf, me).wait_recv()

            if k > 0:
                @pl.when(h + 4 < 2 * N_PHASE * N_COLS)
                def _():
                    dn_start(h + 4)

            if k > 1:
                @pl.when(p == 1)
                def _():
                    gu_start(1, (5, 6) if k == 2 else (7,))

            if k != 1:
                @pl.when(p == 0)
                def _():
                    relay(max(k, 1))

            fold(jnp.maximum(f, 0), f_comb, (src0, src1), kf)
            for i in range(2):
                y = jnp.dot(hid[...], dn[(h + i) % DN_SLOTS], preferred_element_type=F32).astype(BF)
                for half in range(2):
                    buf[work + half, :, k * cw + i * hw : k * cw + (i + 1) * hw] = y[half * cap : (half + 1) * cap]
            y_copy(exp, 2 * side + 1, work + 1, k, base_partner).start()

            @pl.when(side == 1)
            def _():
                y_copy(exp, 2, work, k, base).start()
        return carry

    lax.fori_loop(0, N_PHASE, phase_step, 0)

    for k in range(N_COLS):
        y_copy(1, 1, 1, k, partner).wait_recv()
        fold(0, 0, (0, RECV + 3), k)
    for peer in (2, 3):
        y_copy(1, peer, 0, N_COLS - 1, me).wait_recv()
    fold(3, 3, (RECV + 4, RECV + 5), N_COLS - 1)

    for c in x_copies + m_copies + [p_copy]:
        c.wait_send()
    for exp in range(2):
        for peer in range(1, 4):
            for k in range(N_COLS):
                y_copy(exp, peer, 0, k, devs[peer]).wait_send()


def solution(mesh):
    row_spec = P(("dp", "ep"))

    def local_step(tokens, expert_ids, gate_w, route_counts, w_gate, w_up, w_down):
        tok_n, dim = tokens.shape
        ffn = w_gate.shape[2]
        cap = tok_n // 2
        cw = dim // N_COLS
        vmem = pl.BlockSpec(memory_space=pltpu.VMEM)
        hbm = pl.BlockSpec(memory_space=pl.ANY)
        dma = pltpu.SemaphoreType.DMA
        return pl.pallas_call(
            kernel,
            name="moe",
            out_shape=pltpu.VMEM((tok_n, dim), F32),
            in_specs=[hbm, vmem, vmem, vmem, hbm, hbm, hbm],
            out_specs=vmem,
            scratch_shapes=[
                pltpu.VMEM((RECV + 6, cap, dim), BF),
                pltpu.VMEM((4, 8, tok_n), F32),
                pltpu.VMEM((N_PHASE + 1, 2, tok_n, cap), BF),
                pltpu.VMEM((4, tok_n, 2), F32),
                pltpu.VMEM((2 * cap, ffn), BF),
                pltpu.VMEM((GU_SLOTS, 2, dim, F_BLOCK), BF),
                pltpu.VMEM((DN_SLOTS, ffn, cw // 2), BF),
                dma, dma((GU_SLOTS, 2)), dma((DN_SLOTS,)),
                dma((N_CHUNKS,)), dma((N_CHUNKS,)), dma, dma,
                dma((N_CHUNKS,)), dma((N_CHUNKS,)), dma((3,)), dma((3,)),
                dma((2, 4, N_COLS)), dma((2, 4, N_COLS)),
            ],
            compiler_params=pltpu.CompilerParams(
                collective_id=0, has_side_effects=True, vmem_limit_bytes=64_900_000
            ),
        )(tokens.reshape(2, cap, dim), expert_ids.T, gate_w.T, route_counts, w_gate, w_up, w_down).astype(BF)

    return jax.shard_map(local_step, mesh=mesh, in_specs=(row_spec, row_spec, row_spec, row_spec, P("ep"), P("ep"), P("ep")), out_specs=row_spec, check_vma=False)
```
